512 devices in a mesh: dp: 256 (over y, z_hi, x, core), mp: 2 (over z_lo).
Axes of the slice: x: 4, y: 8, z: 8 (z_hi: 4, z_lo: 2; z = z_hi * 2 + z_lo), core: 2. Of those that a mesh axis runs over, the one named last changes fastest.
Arguments:
- new_embed: bfloat16 [28672, 1280], P('dp'), may hold values from -3 to 3
- context_key_cache: bfloat16 [28672, 16, 1280], P('dp', None, 'mp'), may hold values from -2500 to 2500
- value_cache: bfloat16 [28672, 16, 1280], P('dp', None, 'mp'), may hold values from -6 to 6
- valid: int32 [28672], P('dp'), may hold values from 2 to 16
- attn_gain: float32 [1280], replicated, may hold values from 0.1 to 1.9
- mlp_gain: float32 [1280], replicated, may hold values from 0.1 to 1.9
- query_scale: float32 [80], replicated, may hold values from 0.1 to 1.9
- w_qkv: bfloat16 [3, 1280, 1280], P(None, 'dp', 'mp'), may hold values from -0.15625 to 0.15625
- w_out: bfloat16 [1280, 1280], P('mp', 'dp'), may hold values from -0.625 to 0.625
- w_up: bfloat16 [1280, 1280], P('dp', 'mp'), may hold values from -0.15625 to 0.15625
- w_down: bfloat16 [1280, 1280], P('mp', 'dp'), may hold values from -0.15625 to 0.15625
- head_hidden: bfloat16 [1280, 1280], P('dp', 'mp'), may hold values from -0.15625 to 0.15625
- final_layer_matrices: bfloat16 [2, 1280, 1280], P(None, 'mp', 'dp'), may hold values from -0.15625 to 0.15625
Outputs:
- predicted_levels: float32 [28672, 1280], P('dp', 'mp')
The draws below stay inside these ranges and needn't reach their ends.
Inputs may be any that keep to these rules, and one draw needn't show every extreme that they name: Series s uses its first valid[s] cached patches.
All inputs are finite; a program needn't handle non-finite values.
Results may differ from the reference program's by a relative error of at most 0.035.
Values may be sent and summed in bfloat16 or wider, within the bound.
No kernel may reach another device: no remote copies, remote signals or barrier semaphores. Data moves between devices by JAX's collectives and lax.ppermute only.
A program may use at most 128 MiB of HBM per device.

```python
import math
import jax
import jax.numpy as jnp
from jax import lax

D = 1280
FF = 1280
HEADS = 16
OUT = 1280
SER_DEV = 112
CTX = 16
HD = 80
SERIES = 28672
N_DP = 256


def draw_context_key_cache(key, part):
    base = jnp.clip(jax.random.normal(key, (SERIES, CTX, D), jnp.float32), -6.0, 6.0)
    result = base
    return result.astype(jnp.bfloat16)


def touch_ends(values, stream_key, least, high):
    index_at = [jax.random.randint(jax.random.fold_in(stream_key, axis), (), 0, length) for axis, length in enumerate(values.shape)]
    main_axis = values.shape.index(max(values.shape))
    beside = index_at[:main_axis] + [(index_at[main_axis] + 1) % values.shape[main_axis]] + index_at[main_axis + 1:]
    return values.at[tuple(index_at)].set(least).at[tuple(beside)].set(high)


def block_scale(key, shape, cuts, low, largest):
    def one(position, blocks):
        draws = jax.random.uniform(jax.random.fold_in(jax.random.fold_in(key, 6), position), (blocks,), jnp.float32, low / len(cuts), largest / len(cuts))
        return jnp.repeat(jnp.exp(draws), shape[position] // blocks).reshape((-1,) + (1,) * (len(shape) - position - 1))

    level = one(*cuts[0])
    for cut in cuts[1:]:
        level = level * one(*cut)
    return level


def centred(rng, dims, scale, limit, pieces=(), kind=jnp.bfloat16):
    values = scale * jax.random.normal(rng, dims, jnp.float32)
    if pieces:
        values = values * block_scale(rng, dims, pieces, -0.22, 0.18)
    return jnp.clip(values, -limit, limit).astype(kind)


def setup_inputs(seed: int = 0) -> dict:
    arg_keys = jax.random.split(jax.random.key(seed), 14)
    new_embed = centred(arg_keys[0], (SERIES, D), 0.5, 3.0, ((0, 256),))
    context_key_cache = draw_context_key_cache(jax.random.fold_in(arg_keys[13], 71), 0)
    value_cache = centred(arg_keys[2], (SERIES, CTX, D), 1.0, 6.0, ((0, 256), (2, 2)))
    valid = touch_ends(jax.random.randint(arg_keys[3], (SERIES,), 2, CTX + 1), jax.random.fold_in(arg_keys[3], 1), 2, CTX).astype(jnp.int32)
    attn_gain = jnp.clip(1.0 + 0.18 * jax.random.normal(arg_keys[4], (D,), jnp.float32), 0.1, 1.9)
    mlp_gain = jnp.clip(1.0 + 0.18 * jax.random.normal(arg_keys[5], (D,), jnp.float32), 0.1, 1.9)
    query_scale = jnp.clip(1.0 + 0.18 * jax.random.normal(arg_keys[6], (HD,), jnp.float32), 0.1, 1.9)
    w_qkv = centred(arg_keys[7], (3, D, D), D ** -0.5, 0.15625, ((1, 256), (2, 2)))
    w_out = centred(arg_keys[8], (D, D), (D // 16) ** -0.5, 0.625, ((0, 2), (1, 256)))
    w_up = centred(arg_keys[9], (D, FF), D ** -0.5, 0.15625, ((0, 256), (1, 2)))
    w_down = centred(arg_keys[10], (FF, D), FF ** -0.5, 0.15625, ((0, 2), (1, 256)))
    head_hidden = centred(arg_keys[11], (D, D), D ** -0.5, 0.15625, ((0, 256), (1, 2)))
    final_layer_matrices = centred(arg_keys[12], (2, D, OUT), D ** -0.5, 0.15625, ((1, 2), (2, 256)))
    return dict(new_embed=new_embed, context_key_cache=context_key_cache, value_cache=value_cache, valid=valid, attn_gain=attn_gain, mlp_gain=mlp_gain, query_scale=query_scale, w_qkv=w_qkv, w_out=w_out, w_up=w_up, w_down=w_down, head_hidden=head_hidden, final_layer_matrices=final_layer_matrices)


def rms_scale(values, gain):
    meansq = lax.optimization_barrier(jnp.mean(values * values, axis=-1, keepdims=True))
    return values * lax.rsqrt(meansq + 1e-06) * gain.astype(jnp.float32)

def attend(query_all, key_new, value_new, context_key_cache, value_cache, valid):
    count = context_key_cache.shape[0]
    context_len = context_key_cache.shape[1]
    cache_keys = context_key_cache.reshape(count, context_len, HEADS, HD).astype(jnp.float32)
    cache_vals = value_cache.reshape(count, context_len, HEADS, HD).astype(jnp.float32)
    query_full = query_all.astype(jnp.float32)
    scores = jnp.einsum('bhe,bche->bhc', query_full, cache_keys)
    own_score = lax.optimization_barrier(jnp.sum(query_full * key_new.astype(jnp.float32), axis=-1))
    in_use = jnp.arange(context_len, dtype=jnp.int32)[None, :] < valid[:, None]
    scores = jnp.where(in_use[:, None, :], scores, -jnp.inf)
    highest = jnp.maximum(lax.optimization_barrier(jnp.max(scores, axis=-1)), own_score)
    exp_cache = jnp.exp(scores - highest[..., None])
    exp_own = jnp.exp(own_score - highest)
    denominator = lax.optimization_barrier(jnp.sum(exp_cache, axis=-1)) + exp_own
    weight_cache = (exp_cache / denominator[..., None]).astype(jnp.bfloat16)
    weight_own = (exp_own / denominator).astype(jnp.bfloat16)
    context = jnp.einsum('bhc,bche->bhe', weight_cache.astype(jnp.float32), cache_vals)
    context = context + weight_own.astype(jnp.float32)[..., None] * value_new.astype(jnp.float32)
    return context.astype(jnp.bfloat16).reshape(count, D)

def reference(new_embed, context_key_cache, value_cache, valid, attn_gain, mlp_gain, query_scale, w_qkv, w_out, w_up, w_down, head_hidden, final_layer_matrices):
    stream = new_embed.astype(jnp.float32)
    normed = rms_scale(stream, attn_gain).astype(jnp.bfloat16)
    query_all = jnp.dot(normed, w_qkv[0], preferred_element_type=jnp.float32).reshape(SERIES, HEADS, HD)
    query_all = (query_all * query_scale.astype(jnp.float32) / math.sqrt(HD)).astype(jnp.bfloat16)
    key_new = jnp.dot(normed, w_qkv[1], preferred_element_type=jnp.float32).astype(jnp.bfloat16).reshape(SERIES, HEADS, HD)
    value_new = jnp.dot(normed, w_qkv[2], preferred_element_type=jnp.float32).astype(jnp.bfloat16).reshape(SERIES, HEADS, HD)
    blocked = (query_all.reshape(N_DP, SER_DEV, HEADS, HD), key_new.reshape(N_DP, SER_DEV, HEADS, HD), value_new.reshape(N_DP, SER_DEV, HEADS, HD), context_key_cache.reshape(N_DP, SER_DEV, CTX, D), value_cache.reshape(N_DP, SER_DEV, CTX, D), valid.reshape(N_DP, SER_DEV))
    context = lax.map(lambda items: attend(*items), blocked).reshape(SERIES, D)
    stream1 = stream + jnp.dot(context, w_out, preferred_element_type=jnp.float32)
    normed2 = rms_scale(stream1, mlp_gain).astype(jnp.bfloat16)
    hidden = jax.nn.relu(jnp.dot(normed2, w_up, preferred_element_type=jnp.float32)).astype(jnp.bfloat16)
    carried_signal_second = (stream1 + jnp.dot(hidden, w_down, preferred_element_type=jnp.float32)).astype(jnp.bfloat16)
    quantile_layer_nonlinear = jax.nn.silu(jnp.dot(carried_signal_second, head_hidden, preferred_element_type=jnp.float32)).astype(jnp.bfloat16)
    predicted_levels = jnp.dot(quantile_layer_nonlinear, final_layer_matrices[0], preferred_element_type=jnp.float32)
    predicted_levels = predicted_levels + jnp.dot(carried_signal_second, final_layer_matrices[1], preferred_element_type=jnp.float32)
    return predicted_levels
```

```python
import math

import jax
import jax.numpy as jnp
import numpy as np
from jax import lax
from jax.experimental import pallas as pl
from jax.experimental.pallas import tpu as pltpu
from jax.sharding import Mesh
from jax.sharding import PartitionSpec as P

D = 1280
HEADS = 16
HD = D // HEADS
DP = ("y", "zh", "x", "c")
NY, NZ, NX, NC = 8, 4, 4, 2
PIECE = 5
NEAR = NZ * NX
BLK = NEAR * PIECE
FAR = NY * NC
HIGHEST = lax.Precision.HIGHEST
F32 = jnp.float32
BF16 = jnp.bfloat16


def feature_order():
    f = np.arange(D).reshape(NY, NZ, NX, NC, PIECE)
    return f.transpose(0, 3, 1, 2, 4).reshape(D).astype(np.int32)


def row_pick(places, padded):
    src = (np.arange(NEAR)[None, :, None] * padded + places[:, None, :]).reshape(-1)
    return (src[:, None] == np.arange(NEAR * padded)[None, :]).astype(np.float32)


def gather_blocks(rows, places):
    n, width = rows.shape
    padded = -(-n // 8) * 8
    rows = jnp.pad(rows, ((0, padded - n), (0, 0)))
    copies = jnp.broadcast_to(rows, (NEAR, padded, width))
    near = lax.all_to_all(copies, ("zh", "x"), split_axis=0, concat_axis=0, tiled=True)
    pick = jnp.asarray(row_pick(places, padded), BF16)
    block = jnp.dot(pick, near.reshape(NEAR * padded, width), preferred_element_type=F32)
    block = block.astype(BF16)
    return block, lambda b: lax.all_gather(b, ("y", "c"), axis=0)


def in_hbm(array):
    return pltpu.with_memory_space_constraint(array, pltpu.HBM)


def in_vmem(array):
    return pltpu.with_memory_space_constraint(array, pltpu.VMEM)


def dot(a, b):
    return jnp.dot(a, b, preferred_element_type=F32)


def dot_t(a, b):
    return lax.dot_general(a, b, (((1,), (1,)), ((), ())), preferred_element_type=F32)


def attention_body(
    x_ref, scale_ref, valid_ref, pool_ref, k_buf, v_buf, w_hbm, out_ref,
    w_buf, q_buf, kn_buf, vn_buf, ctx_buf, sems,
):
    rows, width = q_buf.shape
    ctx_len = k_buf.shape[1]
    loads = [
        pltpu.make_async_copy(w_hbm.at[:, pl.ds(b * BLK, BLK), :], w_buf.at[b], sems.at[b])
        for b in range(4)
    ]
    for load in loads:
        load.start()
    x = x_ref[...]
    loads[0].wait()
    q = dot(x, w_buf[0].reshape(D, width))
    q_buf[...] = (q * scale_ref[...] / math.sqrt(HD)).astype(BF16).astype(F32)
    loads[1].wait()
    kn_buf[...] = dot(x, w_buf[1].reshape(D, width)).astype(BF16).astype(F32)
    loads[2].wait()
    vn_buf[...] = dot(x, w_buf[2].reshape(D, width)).astype(BF16).astype(F32)
    pool = pool_ref[...]
    pool_bf = pool.astype(BF16)
    step = 8

    def body(i, carry):
        at = pl.multiple_of(i * step, step)
        q8 = q_buf[pl.ds(at, step), :]
        k8 = k_buf[pl.ds(at, step)].astype(F32)
        prod = (q8[:, None, :] * k8).reshape(step * ctx_len, width)
        scores = jnp.dot(prod, pool, precision=HIGHEST, preferred_element_type=F32)
        own = jnp.dot(
            q8 * kn_buf[pl.ds(at, step), :], pool, precision=HIGHEST, preferred_element_type=F32
        )
        scores = scores.reshape(step, ctx_len, 128)
        used = valid_ref[pl.ds(at, step), :][:, None, :]
        slot = lax.broadcasted_iota(jnp.int32, (step, ctx_len, 128), 1)
        scores = jnp.where(slot < used, scores, -jnp.inf)
        top = jnp.maximum(jnp.max(scores, axis=1), own)
        e_cache = jnp.exp(scores - top[:, None, :])
        e_own = jnp.exp(own - top)
        total = jnp.sum(e_cache, axis=1) + e_own
        w_cache = (e_cache / total[:, None, :]).astype(BF16).reshape(step * ctx_len, 128)
        w_own = (e_own / total).astype(BF16)
        wide = dot_t(w_cache, pool_bf).reshape(step, ctx_len, width)
        v8 = v_buf[pl.ds(at, step)].astype(F32)
        ctx = jnp.sum(wide * v8, axis=1)
        ctx_buf[pl.ds(at, step), :] = ctx + dot_t(w_own, pool_bf) * vn_buf[pl.ds(at, step), :]
        return carry

    lax.fori_loop(0, rows // step, body, 0)
    loads[3].wait()
    out_ref[...] = dot_t(ctx_buf[...].astype(BF16), w_buf[3].reshape(D, width)).astype(BF16)


def attention_kernel(x, scale, valid, pool, keys, vals, w):
    rows, ctx_len, width = keys.shape
    vmem = pl.BlockSpec(memory_space=pltpu.VMEM)
    hbm = pl.BlockSpec(memory_space=pltpu.HBM)
    return pl.pallas_call(
        attention_body,
        out_shape=pltpu.VMEM((rows, D), BF16),
        in_specs=[vmem, vmem, vmem, vmem, vmem, vmem, hbm],
        out_specs=vmem,
        scratch_shapes=[
            pltpu.VMEM((4, FAR, BLK, width), BF16),
            pltpu.VMEM((rows, width), F32),
            pltpu.VMEM((rows, width), F32),
            pltpu.VMEM((rows, width), F32),
            pltpu.VMEM((rows, width), F32),
            pltpu.SemaphoreType.DMA((4,)),
        ],
        compiler_params=pltpu.CompilerParams(vmem_limit_bytes=48 * 2**20),
        name="attend",
    )(x, scale, valid, pool, in_vmem(keys), in_vmem(vals), in_hbm(w))


def mlp_body(stream_ref, own_ref, other_ref, gain_ref, w_hbm, s1_ref, out_ref, w_buf, sems):
    loads = [
        pltpu.make_async_copy(w_hbm.at[:, pl.ds((4 + b) * BLK, BLK), :], w_buf.at[b], sems.at[b])
        for b in range(2)
    ]
    for load in loads:
        load.start()
    width = w_buf.shape[-1]
    s1 = stream_ref[...].astype(F32) + (own_ref[...].astype(F32) + other_ref[...].astype(F32))
    s1_ref[...] = s1
    meansq = jnp.mean(s1 * s1, axis=-1, keepdims=True)
    n2 = (s1 * lax.rsqrt(meansq + 1e-06) * gain_ref[...]).astype(BF16)
    loads[0].wait()
    hidden = jnp.maximum(dot(n2, w_buf[0].reshape(D, width)), 0.0).astype(BF16)
    loads[1].wait()
    out_ref[...] = dot_t(hidden, w_buf[1].reshape(D, width)).astype(BF16)


def mlp_kernel(stream, own, other, gain, w):
    rows = stream.shape[0]
    vmem = pl.BlockSpec(memory_space=pltpu.VMEM)
    hbm = pl.BlockSpec(memory_space=pltpu.HBM)
    return pl.pallas_call(
        mlp_body,
        out_shape=(pltpu.VMEM((rows, D), F32), pltpu.VMEM((rows, D), BF16)),
        in_specs=[vmem, vmem, vmem, vmem, hbm],
        out_specs=(vmem, vmem),
        scratch_shapes=[
            pltpu.VMEM((2, FAR, BLK, w.shape[-1]), BF16),
            pltpu.SemaphoreType.DMA((2,)),
        ],
        compiler_params=pltpu.CompilerParams(vmem_limit_bytes=32 * 2**20),
        name="mlp",
    )(stream, own, other, gain, in_hbm(w))


def head_body(s1_ref, own_ref, other_ref, back_ref, w_hbm, mine_ref, give_ref, w_buf, sems):
    loads = [
        pltpu.make_async_copy(w_hbm.at[:, pl.ds(b * BLK, BLK), :], w_buf.at[b], sems.at[b])
        for b in range(3)
    ]
    for load in loads:
        load.start()
    width = w_buf.shape[-1]
    feed = own_ref[...].astype(F32) + other_ref[...].astype(F32)
    s2 = (s1_ref[...] + feed).astype(BF16)
    s2_half = dot(s2, back_ref[:, :width]).astype(BF16)
    loads[0].wait()
    pre = dot(s2, w_buf[0].reshape(D, width))
    act = (pre / (1.0 + jnp.exp(-pre))).astype(BF16)
    loads[1].wait()
    out = dot_t(act, w_buf[1].reshape(D, width))
    loads[2].wait()
    out = (out + dot_t(s2_half, w_buf[2].reshape(D, width))).astype(BF16)
    give_ref[...] = dot(out, back_ref[:, width:]).astype(BF16)
    mine_ref[...] = dot(out, back_ref[:, :width]).astype(BF16)


def head_kernel(s1, own, other, back, w):
    rows = s1.shape[0]
    width = w.shape[-1]
    vmem = pl.BlockSpec(memory_space=pltpu.VMEM)
    hbm = pl.BlockSpec(memory_space=pltpu.HBM)
    half = pltpu.VMEM((rows, width), BF16)
    return pl.pallas_call(
        head_body,
        out_shape=(half, half),
        in_specs=[vmem, vmem, vmem, vmem, hbm],
        out_specs=(vmem, vmem),
        scratch_shapes=[pltpu.VMEM((3, FAR, BLK, width), BF16), pltpu.SemaphoreType.DMA((3,))],
        compiler_params=pltpu.CompilerParams(vmem_limit_bytes=32 * 2**20),
        name="head",
    )(s1, own, other, in_vmem(back), in_hbm(w))


def rms_scale(values, gain):
    meansq = jnp.mean(values * values, axis=-1, keepdims=True)
    return values * lax.rsqrt(meansq + 1e-06) * gain


def swap(array):
    return lax.ppermute(array, "mp", [(0, 1), (1, 0)])


def per_device(
    new_embed,
    context_key_cache,
    value_cache,
    valid,
    attn_gain,
    mlp_gain,
    query_scale,
    w_qkv,
    w_out,
    w_up,
    w_down,
    head_hidden,
    final_layer_matrices,
):
    rows, _, width = context_key_cache.shape
    heads = width // HD
    first = jnp.concatenate(
        [
            jnp.transpose(w_qkv, (1, 0, 2)).reshape(3 * PIECE, width),
            w_out.T,
            w_up,
            w_down.T,
        ],
        axis=0,
    )
    piece = np.arange(PIECE)
    first_places = np.stack([piece * 3 + b for b in range(3)] + [piece + PIECE * b for b in range(3, 6)])
    block1, gather1 = gather_blocks(first, first_places)
    block1, head_hidden, final_layer_matrices = lax.optimization_barrier(
        (block1, head_hidden, final_layer_matrices)
    )
    all1 = gather1(block1)
    second = jnp.concatenate(
        [head_hidden, jnp.transpose(final_layer_matrices, (0, 2, 1)).reshape(2 * PIECE, width)],
        axis=0,
    )
    block2, gather2 = gather_blocks(second, np.stack([piece + PIECE * b for b in range(3)]))
    all2 = gather2(block2)

    order = jnp.asarray(feature_order())
    ids = jnp.arange(D, dtype=jnp.int32)
    forth = (ids[:, None] == order[None, :]).astype(BF16)
    at = (ids + lax.axis_index("mp") * width) % D
    back = (order[:, None] == at[None, :]).astype(BF16)

    normed = rms_scale(new_embed.astype(F32), attn_gain).astype(BF16)
    both = jnp.dot(jnp.concatenate([normed, new_embed], axis=0), forth, preferred_element_type=F32)
    both = both.astype(BF16)
    normed_o, stream_o = both[:rows], both[rows:]
    gain_o = mlp_gain.reshape(NY, NZ, NX, NC, PIECE).transpose(0, 3, 1, 2, 4).reshape(1, D)
    pool = (jnp.arange(width)[:, None] // HD == jnp.arange(128)[None, :]).astype(F32)
    scale = jnp.tile(query_scale, heads).reshape(1, width)
    used = jnp.broadcast_to(valid[:, None], (rows, 128))

    part = attention_kernel(
        normed_o, scale, used, pool, context_key_cache, value_cache, all1
    )
    stream1, feed = mlp_kernel(stream_o, part, swap(part), gain_o, all1)
    mine, give = head_kernel(stream1, feed, swap(feed), back, all2)
    return mine.astype(F32) + swap(give).astype(F32)


def solution(mesh):
    split = Mesh(
        mesh.devices.reshape(NY, NZ, NX, NC, mesh.shape["mp"]), ("y", "zh", "x", "c", "mp")
    )
    return jax.shard_map(
        per_device,
        mesh=split,
        in_specs=(
            P(DP, None),
            P(DP, None, "mp"),
            P(DP, None, "mp"),
            P(DP),
            P(),
            P(),
            P(),
            P(None, DP, "mp"),
            P("mp", DP),
            P(DP, "mp"),
            P("mp", DP),
            P(DP, "mp"),
            P(None, "mp", DP),
        ),
        out_specs=P(DP, "mp"),
        check_vma=False,
    )
```

```python
import math

import jax
import jax.numpy as jnp
import numpy as np
from jax import lax
from jax.experimental import pallas as pl
from jax.experimental.pallas import tpu as pltpu
from jax.sharding import Mesh
from jax.sharding import PartitionSpec as P

D = 1280
HEADS = 16
HD = D // HEADS
DP = ("y", "zh", "x", "c")
NY, NZ, NX, NC = 8, 4, 4, 2
PIECE = 5
NEAR = NZ * NX
BLK = NEAR * PIECE
FAR = NY * NC
STEP = 56
F32 = jnp.float32
BF16 = jnp.bfloat16


def feature_order():
    f = np.arange(D).reshape(NY, NZ, NX, NC, PIECE)
    return f.transpose(0, 3, 1, 2, 4).reshape(D).astype(np.int32)


def half_order():
    f = np.arange(D).reshape(NY, NZ, NX, NC, PIECE)[:, :, :, 0]
    return f.transpose(2, 0, 1, 3).reshape(D // NC).astype(np.int32)


def row_pick(places, near, padded):
    src = (np.arange(near)[None, :, None] * padded + places[:, None, :]).reshape(-1)
    return jnp.asarray(src[:, None] == np.arange(near * padded)[None, :], BF16)


def padded_rows(parts):
    rows = jnp.concatenate(parts, axis=0)
    return jnp.pad(rows, ((0, -rows.shape[0] % 8), (0, 0)))


def from_all(array, axis):
    copies = jnp.broadcast_to(array, (lax.axis_size(axis), *array.shape))
    return lax.all_to_all(copies, axis, split_axis=0, concat_axis=0, tiled=True)


def in_hbm(array):
    return pltpu.with_memory_space_constraint(array, pltpu.HBM)


def in_vmem(array):
    return pltpu.with_memory_space_constraint(array, pltpu.VMEM)


def dot(a, b):
    return jnp.dot(a, b, preferred_element_type=F32)


def dot_t(a, b):
    return lax.dot_general(a, b, (((1,), (1,)), ((), ())), preferred_element_type=F32)


def attention_body(
    x_ref, scale_ref, valid_ref, pool_ref, k_ref, vals_hbm, w_hbm, out_ref,
    w_buf, v_buf, q_buf, kn_buf, vn_buf, ctx_buf, sems,
):
    rows, width = q_buf.shape
    ctx_len = k_ref.shape[1]
    loads = [
        pltpu.make_async_copy(w_hbm.at[:, pl.ds(b * BLK, BLK), :], w_buf.at[b], sems.at[b])
        for b in range(4)
    ]
    load_v = pltpu.make_async_copy(vals_hbm, v_buf, sems.at[4])
    for load in loads[:3]:
        load.start()
    load_v.start()
    loads[3].start()
    x = x_ref[...]
    loads[0].wait()
    q = dot(x, w_buf[0].reshape(D, width))
    q_buf[...] = (q * scale_ref[...] / math.sqrt(HD)).astype(BF16).astype(F32)
    loads[1].wait()
    kn_buf[...] = dot(x, w_buf[1].reshape(D, width)).astype(BF16).astype(F32)
    loads[2].wait()
    vn_buf[...] = dot(x, w_buf[2].reshape(D, width)).astype(BF16).astype(F32)
    load_v.wait()
    pool = pool_ref[...]
    step = STEP

    def head_sums(prod):
        high = prod.astype(BF16)
        low = (prod - high.astype(F32)).astype(BF16)
        return dot(high, pool) + dot(low, pool)

    def body(i, carry):
        at = pl.multiple_of(i * step, 8)
        q8 = q_buf[pl.ds(at, step), :]
        k8 = k_ref[pl.ds(at, step)].astype(F32)
        prod = (q8[:, None, :] * k8).reshape(step * ctx_len, width)
        scores = head_sums(prod).reshape(step, ctx_len, 128)
        own = head_sums(q8 * kn_buf[pl.ds(at, step), :])
        used = valid_ref[pl.ds(at, step), :][:, None, :]
        slot = lax.broadcasted_iota(jnp.int32, (step, ctx_len, 128), 1)
        scores = jnp.where(slot < used, scores, -jnp.inf)
        top = jnp.maximum(jnp.max(scores, axis=1), own)
        e_cache = jnp.exp(scores - top[:, None, :])
        e_own = jnp.exp(own - top)
        total = jnp.sum(e_cache, axis=1) + e_own
        w_cache = (e_cache / total[:, None, :]).astype(BF16).reshape(step * ctx_len, 128)
        w_own = (e_own / total).astype(BF16)
        wide = dot_t(w_cache, pool).reshape(step, ctx_len, width)
        v8 = v_buf[pl.ds(at, step)].astype(F32)
        ctx = jnp.sum(wide * v8, axis=1)
        ctx_buf[pl.ds(at, step), :] = ctx + dot_t(w_own, pool) * vn_buf[pl.ds(at, step), :]
        return carry

    lax.fori_loop(0, rows // step, body, 0)
    loads[3].wait()
    out_ref[...] = dot_t(ctx_buf[...].astype(BF16), w_buf[3].reshape(D, width)).astype(BF16)


def attention_kernel(x, scale, valid, pool, keys, vals, w):
    rows, ctx_len, width = keys.shape
    vmem = pl.BlockSpec(memory_space=pltpu.VMEM)
    hbm = pl.BlockSpec(memory_space=pltpu.HBM)
    return pl.pallas_call(
        attention_body,
        out_shape=pltpu.VMEM((rows, D), BF16),
        in_specs=[vmem, vmem, vmem, vmem, vmem, hbm, hbm],
        out_specs=vmem,
        scratch_shapes=[
            pltpu.VMEM((4, FAR, BLK, width), BF16),
            pltpu.VMEM((rows, ctx_len, width), BF16),
            pltpu.VMEM((rows, width), F32),
            pltpu.VMEM((rows, width), F32),
            pltpu.VMEM((rows, width), F32),
            pltpu.VMEM((rows, width), F32),
            pltpu.SemaphoreType.DMA((5,)),
        ],
        compiler_params=pltpu.CompilerParams(vmem_limit_bytes=48 * 2**20),
        name="attend",
    )(x, scale, valid, pool, in_vmem(keys), in_hbm(vals), in_hbm(w))


def mlp_body(stream_ref, own_ref, other_ref, gain_ref, w_hbm, out_ref, w_buf, sems):
    loads = [
        pltpu.make_async_copy(w_hbm.at[:, pl.ds((4 + b) * BLK, BLK), :], w_buf.at[b], sems.at[b])
        for b in range(2)
    ]
    for load in loads:
        load.start()
    width = w_buf.shape[-1]
    s1 = stream_ref[...].astype(F32) + (own_ref[...].astype(F32) + other_ref[...].astype(F32))
    meansq = jnp.mean(s1 * s1, axis=-1, keepdims=True)
    n2 = (s1 * lax.rsqrt(meansq + 1e-06) * gain_ref[...]).astype(BF16)
    loads[0].wait()
    hidden = jnp.maximum(dot(n2, w_buf[0].reshape(D, width)), 0.0).astype(BF16)
    loads[1].wait()
    out_ref[...] = dot_t(hidden, w_buf[1].reshape(D, width)).astype(BF16)


def mlp_kernel(stream, own, other, gain, w):
    rows = stream.shape[0]
    vmem = pl.BlockSpec(memory_space=pltpu.VMEM)
    hbm = pl.BlockSpec(memory_space=pltpu.HBM)
    return pl.pallas_call(
        mlp_body,
        out_shape=pltpu.VMEM((rows, D), BF16),
        in_specs=[vmem, vmem, vmem, vmem, hbm],
        out_specs=vmem,
        scratch_shapes=[
            pltpu.VMEM((2, FAR, BLK, w.shape[-1]), BF16),
            pltpu.SemaphoreType.DMA((2,)),
        ],
        compiler_params=pltpu.CompilerParams(vmem_limit_bytes=32 * 2**20),
        name="mlp",
    )(stream, own, other, gain, in_hbm(w))


def head_body(
    stream_ref, own1_ref, other1_ref, own2_ref, other2_ref, far_ref, turn_hbm, back_hbm, near_hbm,
    mine_ref, give_ref, turn_buf, back_buf, w_buf, sems,
):
    width = w_buf.shape[-1]
    half = D // NC
    each = half // NX

    def rows(b):
        return pl.ds(b * each, each)

    def far(b):
        return far_ref[:, rows(b), :].reshape(half, width)

    def near(b):
        return w_buf[b].reshape(half, width)

    load_turn = pltpu.make_async_copy(turn_hbm, turn_buf, sems.at[0])
    load_back = pltpu.make_async_copy(back_hbm, back_buf, sems.at[1])
    loads = [
        pltpu.make_async_copy(near_hbm.at[:, rows(b), :], w_buf.at[b], sems.at[2 + b])
        for b in range(3)
    ]
    load_turn.start()
    loads[0].start()
    load_back.start()
    loads[1].start()
    loads[2].start()
    s1 = stream_ref[...].astype(F32) + (own1_ref[...].astype(F32) + other1_ref[...].astype(F32))
    s2 = (s1 + (own2_ref[...].astype(F32) + other2_ref[...].astype(F32))).astype(BF16)
    load_turn.wait()
    s2 = dot(s2, turn_buf[...]).astype(BF16)
    loads[0].wait()
    pre = dot(s2[:, :half], near(0)) + dot(s2[:, half:], far(0))
    act = (pre / (1.0 + jnp.exp(-pre))).astype(BF16)
    load_back.wait()
    s2_half = dot(s2, back_buf[:, :width]).astype(BF16)
    loads[1].wait()
    loads[2].wait()
    out = [dot_t(act, w(1)) + dot_t(s2_half, w(2)) for w in (near, far)]
    out = jnp.concatenate(out, axis=1).astype(BF16)
    give_ref[...] = dot(out, back_buf[:, width:]).astype(BF16)
    mine_ref[...] = dot(out, back_buf[:, :width]).astype(BF16)


def head_kernel(stream, own1, other1, own2, other2, turn, back, near, far):
    rows = stream.shape[0]
    width = near.shape[-1]
    vmem = pl.BlockSpec(memory_space=pltpu.VMEM)
    hbm = pl.BlockSpec(memory_space=pltpu.HBM)
    half = pltpu.VMEM((rows, width), BF16)
    return pl.pallas_call(
        head_body,
        out_shape=(half, half),
        in_specs=[vmem, vmem, vmem, vmem, vmem, vmem, hbm, hbm, hbm],
        out_specs=(vmem, vmem),
        scratch_shapes=[
            pltpu.VMEM((D, D), BF16),
            pltpu.VMEM((D, D), BF16),
            pltpu.VMEM((3, NX, D // NC // NX, width), BF16),
            pltpu.SemaphoreType.DMA((5,)),
        ],
        compiler_params=pltpu.CompilerParams(vmem_limit_bytes=32 * 2**20),
        name="head",
    )(stream, own1, other1, own2, other2, in_vmem(far), in_hbm(turn), in_hbm(back), in_hbm(near))


def rms_scale(values, gain):
    meansq = jnp.mean(values * values, axis=-1, keepdims=True)
    return values * lax.rsqrt(meansq + 1e-06) * gain


def swap(array):
    return lax.ppermute(array, "mp", [(0, 1), (1, 0)])


def per_device(
    new_embed,
    context_key_cache,
    value_cache,
    valid,
    attn_gain,
    mlp_gain,
    query_scale,
    w_qkv,
    w_out,
    w_up,
    w_down,
    head_hidden,
    final_layer_matrices,
):
    rows, _, width = context_key_cache.shape
    heads = width // HD
    piece = np.arange(PIECE)
    first = padded_rows(
        [jnp.transpose(w_qkv, (1, 0, 2)).reshape(3 * PIECE, width), w_out.T, w_up, w_down.T]
    )
    places = np.stack([piece * 3 + b for b in range(3)] + [piece + PIECE * b for b in range(3, 6)])
    shared = from_all(first, ("zh", "x")).reshape(-1, width)
    block1 = dot(row_pick(places, NEAR, first.shape[0]), shared).astype(BF16)
    block1, head_hidden, final_layer_matrices = lax.optimization_barrier(
        (block1, head_hidden, final_layer_matrices)
    )
    all1 = lax.all_gather(block1, ("y", "c"), axis=0)
    second = padded_rows(
        [head_hidden, jnp.transpose(final_layer_matrices, (0, 2, 1)).reshape(2 * PIECE, width)]
    )
    shared = from_all(second, "zh").reshape(-1, width)
    shared, new_embed = lax.optimization_barrier((shared, new_embed))
    shared = from_all(shared, "y").reshape(-1, width)
    places = np.stack([piece + PIECE * b for b in range(3)])
    block2 = dot(row_pick(places, NY * NZ, second.shape[0]), shared).astype(BF16)

    core = lax.axis_index("c")
    order = jnp.asarray(feature_order())
    half = jnp.asarray(half_order())
    order2 = jnp.concatenate([half + PIECE * core, half + PIECE * (1 - core)])
    ids = jnp.arange(D, dtype=jnp.int32)
    at = (ids + lax.axis_index("mp") * width) % D
    forth = (ids[:, None] == order[None, :]).astype(BF16)
    turn = (order[:, None] == order2[None, :]).astype(BF16)
    back = (order2[:, None] == at[None, :]).astype(BF16)

    normed = rms_scale(new_embed.astype(F32), attn_gain).astype(BF16)
    both = dot(jnp.concatenate([normed, new_embed], axis=0), forth).astype(BF16)
    normed_o, stream_o = both[:rows], both[rows:]
    gain_o = mlp_gain.reshape(NY, NZ, NX, NC, PIECE).transpose(0, 3, 1, 2, 4).reshape(1, D)
    pool = (jnp.arange(width)[:, None] // HD == jnp.arange(128)[None, :]).astype(BF16)
    scale = jnp.tile(query_scale, heads).reshape(1, width)
    used = jnp.broadcast_to(valid[:, None], (rows, 128))
    normed_o, stream_o, gain_o, pool, scale, used, turn, back, block2 = lax.optimization_barrier(
        (normed_o, stream_o, gain_o, pool, scale, used, turn, back, block2)
    )
    near = from_all(block2, "x")
    far = lax.ppermute(near, "c", [(0, 1), (1, 0)])

    part1 = attention_kernel(
        normed_o, scale, used, pool, context_key_cache, value_cache, all1
    )
    other1 = swap(part1)
    part2 = mlp_kernel(stream_o, part1, other1, gain_o, all1)
    mine, give = head_kernel(
        stream_o, part1, other1, part2, swap(part2), turn, back, near, far
    )
    return mine.astype(F32) + swap(give).astype(F32)


def solution(mesh):
    split = Mesh(
        mesh.devices.reshape(NY, NZ, NX, NC, mesh.shape["mp"]), ("y", "zh", "x", "c", "mp")
    )

    return jax.shard_map(
        per_device,
        mesh=split,
        in_specs=(
            P(DP, None),
            P(DP, None, "mp"),
            P(DP, None, "mp"),
            P(DP),
            P(),
            P(),
            P(),
            P(None, DP, "mp"),
            P("mp", DP),
            P(DP, "mp"),
            P("mp", DP),
            P(DP, "mp"),
            P(None, "mp", DP),
        ),
        out_specs=P(DP, "mp"),
        check_vma=False,
    )
```

```python
import math

import jax
import jax.numpy as jnp
import numpy as np
from jax import lax
from jax.experimental import pallas as pl
from jax.experimental.pallas import tpu as pltpu
from jax.sharding import Mesh
from jax.sharding import PartitionSpec as P

D = 1280
HEADS = 16
HD = D // HEADS
DP = ("y", "zh", "x", "c")
NY, NZ, NX, NC = 8, 4, 4, 2
PIECE = 5
NEAR = NZ * NX
BLK = NEAR * PIECE
FAR = NY * NC
STEP = 56
F32 = jnp.float32
BF16 = jnp.bfloat16


def feature_order():
    f = np.arange(D).reshape(NY, NZ, NX, NC, PIECE)
    return f.transpose(0, 3, 1, 2, 4).reshape(D).astype(np.int32)


def half_order():
    f = np.arange(D).reshape(NY, NZ, NX, NC, PIECE)[:, :, :, 0]
    return f.transpose(2, 1, 0, 3).reshape(D // NC).astype(np.int32)


def output_order():
    f = np.arange(D // 2).reshape(NY // 2, NZ, NX, NC, PIECE)[:, :, :, 0]
    return f.transpose(2, 1, 0, 3).reshape(D // 2 // NC).astype(np.int32)


def output_rows(padded):
    zh, y, piece = np.meshgrid(np.arange(NZ), np.arange(NY), np.arange(PIECE), indexing="ij")

    def at(slot, row):
        return (zh * NY + slot) * padded + row + piece

    def halves(row):
        src = at(y, row)
        return np.concatenate([src[:, : NY // 2].reshape(-1), src[:, NY // 2 :].reshape(-1)])

    own = at(y, 0).reshape(-1)
    other = at((y + NY // 2) % NY, PIECE).reshape(-1)
    return np.concatenate([own, other, halves(2 * PIECE), halves(3 * PIECE)])


def row_pick(places, near, padded):
    src = (np.arange(near)[None, :, None] * padded + places[:, None, :]).reshape(-1)
    return one_hot(src, near * padded)


def one_hot(src, count):
    src = jnp.asarray(src.astype(np.int32))
    return (src[:, None] == jnp.arange(count, dtype=jnp.int32)[None, :]).astype(BF16)


def padded_rows(parts):
    rows = jnp.concatenate(parts, axis=0)
    return jnp.pad(rows, ((0, -rows.shape[0] % 8), (0, 0)))


def from_all(array, axis):
    copies = jnp.broadcast_to(array, (lax.axis_size(axis), *array.shape))
    return lax.all_to_all(copies, axis, split_axis=0, concat_axis=0, tiled=True)


def in_hbm(array):
    return pltpu.with_memory_space_constraint(array, pltpu.HBM)


def in_vmem(array):
    return pltpu.with_memory_space_constraint(array, pltpu.VMEM)


def dot(a, b):
    return jnp.dot(a, b, preferred_element_type=F32)


def dot_t(a, b):
    return lax.dot_general(a, b, (((1,), (1,)), ((), ())), preferred_element_type=F32)


def attention_body(
    x_ref, scale_ref, valid_ref, pool_ref, k_ref, vals_hbm, w_hbm, out_ref,
    w_buf, v_buf, q_buf, kn_buf, vn_buf, ctx_buf, sems,
):
    rows, width = q_buf.shape
    ctx_len = k_ref.shape[1]
    loads = [
        pltpu.make_async_copy(w_hbm.at[:, pl.ds(b * BLK, BLK), :], w_buf.at[b], sems.at[b])
        for b in range(4)
    ]
    load_v = pltpu.make_async_copy(vals_hbm, v_buf, sems.at[4])
    for load in loads[:3]:
        load.start()
    load_v.start()
    loads[3].start()
    x = x_ref[...]
    loads[0].wait()
    q = dot(x, w_buf[0].reshape(D, width))
    q_buf[...] = (q * scale_ref[...] / math.sqrt(HD)).astype(BF16).astype(F32)
    loads[1].wait()
    kn_buf[...] = dot(x, w_buf[1].reshape(D, width)).astype(BF16).astype(F32)
    loads[2].wait()
    vn_buf[...] = dot(x, w_buf[2].reshape(D, width)).astype(BF16).astype(F32)
    load_v.wait()
    pool = pool_ref[...]
    step = STEP

    def head_sums(prod):
        high = prod.astype(BF16)
        low = (prod - high.astype(F32)).astype(BF16)
        return dot(high, pool) + dot(low, pool)

    def body(i, carry):
        at = pl.multiple_of(i * step, 8)
        q8 = q_buf[pl.ds(at, step), :]
        k8 = k_ref[pl.ds(at, step)].astype(F32)
        prod = (q8[:, None, :] * k8).reshape(step * ctx_len, width)
        scores = head_sums(prod).reshape(step, ctx_len, 128)
        own = head_sums(q8 * kn_buf[pl.ds(at, step), :])
        used = valid_ref[pl.ds(at, step), :][:, None, :]
        slot = lax.broadcasted_iota(jnp.int32, (step, ctx_len, 128), 1)
        scores = jnp.where(slot < used, scores, -jnp.inf)
        top = jnp.maximum(jnp.max(scores, axis=1), own)
        e_cache = jnp.exp(scores - top[:, None, :])
        e_own = jnp.exp(own - top)
        total = jnp.sum(e_cache, axis=1) + e_own
        w_cache = (e_cache / total[:, None, :]).astype(BF16).reshape(step * ctx_len, 128)
        w_own = (e_own / total).astype(BF16)
        wide = dot_t(w_cache, pool).reshape(step, ctx_len, width)
        v8 = v_buf[pl.ds(at, step)].astype(F32)
        ctx = jnp.sum(wide * v8, axis=1)
        ctx_buf[pl.ds(at, step), :] = ctx + dot_t(w_own, pool) * vn_buf[pl.ds(at, step), :]
        return carry

    lax.fori_loop(0, rows // step, body, 0)
    loads[3].wait()
    out_ref[...] = dot_t(ctx_buf[...].astype(BF16), w_buf[3].reshape(D, width)).astype(BF16)


def attention_kernel(x, scale, valid, pool, keys, vals, w):
    rows, ctx_len, width = keys.shape
    vmem = pl.BlockSpec(memory_space=pltpu.VMEM)
    hbm = pl.BlockSpec(memory_space=pltpu.HBM)
    return pl.pallas_call(
        attention_body,
        out_shape=pltpu.VMEM((rows, D), BF16),
        in_specs=[vmem, vmem, vmem, vmem, vmem, hbm, hbm],
        out_specs=vmem,
        scratch_shapes=[
            pltpu.VMEM((4, FAR, BLK, width), BF16),
            pltpu.VMEM((rows, ctx_len, width), BF16),
            pltpu.VMEM((rows, width), F32),
            pltpu.VMEM((rows, width), F32),
            pltpu.VMEM((rows, width), F32),
            pltpu.VMEM((rows, width), F32),
            pltpu.SemaphoreType.DMA((5,)),
        ],
        compiler_params=pltpu.CompilerParams(vmem_limit_bytes=48 * 2**20),
        name="attend",
    )(x, scale, valid, pool, in_vmem(keys), in_hbm(vals), in_hbm(w))


def mlp_body(stream_ref, own_ref, other_ref, gain_ref, w_hbm, out_ref, w_buf, sems):
    loads = [
        pltpu.make_async_copy(w_hbm.at[:, pl.ds((4 + b) * BLK, BLK), :], w_buf.at[b], sems.at[b])
        for b in range(2)
    ]
    for load in loads:
        load.start()
    width = w_buf.shape[-1]
    s1 = stream_ref[...].astype(F32) + (own_ref[...].astype(F32) + other_ref[...].astype(F32))
    meansq = jnp.mean(s1 * s1, axis=-1, keepdims=True)
    n2 = (s1 * lax.rsqrt(meansq + 1e-06) * gain_ref[...]).astype(BF16)
    loads[0].wait()
    hidden = jnp.maximum(dot(n2, w_buf[0].reshape(D, width)), 0.0).astype(BF16)
    loads[1].wait()
    out_ref[...] = dot_t(hidden, w_buf[1].reshape(D, width)).astype(BF16)


def mlp_kernel(stream, own, other, gain, w):
    rows = stream.shape[0]
    vmem = pl.BlockSpec(memory_space=pltpu.VMEM)
    hbm = pl.BlockSpec(memory_space=pltpu.HBM)
    return pl.pallas_call(
        mlp_body,
        out_shape=pltpu.VMEM((rows, D), BF16),
        in_specs=[vmem, vmem, vmem, vmem, hbm],
        out_specs=vmem,
        scratch_shapes=[
            pltpu.VMEM((2, FAR, BLK, w.shape[-1]), BF16),
            pltpu.SemaphoreType.DMA((2,)),
        ],
        compiler_params=pltpu.CompilerParams(vmem_limit_bytes=32 * 2**20),
        name="mlp",
    )(stream, own, other, gain, in_hbm(w))


def head_body(
    stream_ref, own1_ref, other1_ref, own2_ref, other2_ref, first_ref, far_ref,
    turn_hbm, plain_hbm, last_hbm, near_hbm,
    out_ref, turn_buf, plain_buf, last_buf, near_ref, sems,
):
    width = near_ref.shape[-1]
    half = D // NC
    each = half // NX
    copies = [
        pltpu.make_async_copy(src, dst, sems.at[n])
        for n, (src, dst) in enumerate(
            (
                (turn_hbm, turn_buf),
                (near_hbm, near_ref),
                (plain_hbm, plain_buf),
                (last_hbm, last_buf),
            )
        )
    ]
    for copy in copies:
        copy.start()

    def part(ref, start, count):
        return ref[:, pl.ds(start, count), :].reshape(NX * count, width)

    s1 = stream_ref[...].astype(F32) + (own1_ref[...].astype(F32) + other1_ref[...].astype(F32))
    s2 = (s1 + (own2_ref[...].astype(F32) + other2_ref[...].astype(F32))).astype(BF16)
    copies[0].wait()
    turned = dot(s2, turn_buf[...]).astype(BF16)
    copies[1].wait()

    def hidden(start):
        pre = dot(turned[:, :half], part(near_ref, start, each))
        pre = pre + dot(turned[:, half:], part(far_ref, start, each))
        return (pre / (1.0 + jnp.exp(-pre))).astype(BF16)

    act_own = hidden(0)
    act_other = hidden(each)
    first = first_ref[...] > 0
    act = (jnp.where(first, act_own, act_other), jnp.where(first, act_other, act_own))
    copies[2].wait()
    plain = dot(s2, plain_buf[...]).astype(BF16)
    skip = (plain[:, :width], plain[:, width:])
    out = []
    for ref in (near_ref, far_ref):
        total = None
        for k in range(2):
            at = 2 * each + k * (each // 2)
            term = dot_t(act[k], part(ref, at, each // 2))
            term = term + dot_t(skip[k], part(ref, at + each, each // 2))
            total = term if total is None else total + term
        out.append(total)
    out = jnp.concatenate(out, axis=1)
    high = out.astype(BF16)
    low = (out - high.astype(F32)).astype(BF16)
    copies[3].wait()
    out_ref[...] = dot(high, last_buf[...]) + dot(low, last_buf[...])


def head_kernel(stream, own1, other1, own2, other2, first, turn, plain, last, near, far):
    rows = stream.shape[0]
    width = near.shape[-1]
    vmem = pl.BlockSpec(memory_space=pltpu.VMEM)
    hbm = pl.BlockSpec(memory_space=pltpu.HBM)
    return pl.pallas_call(
        head_body,
        out_shape=jax.ShapeDtypeStruct((rows, width), F32),
        in_specs=[vmem] * 7 + [hbm] * 4,
        out_specs=vmem,
        scratch_shapes=[
            pltpu.VMEM(turn.shape, BF16),
            pltpu.VMEM(plain.shape, BF16),
            pltpu.VMEM(last.shape, BF16),
            pltpu.VMEM(near.shape, BF16),
            pltpu.SemaphoreType.DMA((4,)),
        ],
        compiler_params=pltpu.CompilerParams(vmem_limit_bytes=32 * 2**20),
        name="head",
    )(
        stream, own1, other1, own2, other2, first, in_vmem(far),
        in_hbm(turn), in_hbm(plain), in_hbm(last), in_hbm(near),
    )


def rms_scale(values, gain):
    meansq = jnp.mean(values * values, axis=-1, keepdims=True)
    return values * lax.rsqrt(meansq + 1e-06) * gain


def swap(array):
    return lax.ppermute(array, "mp", [(0, 1), (1, 0)])


def per_device(
    new_embed,
    context_key_cache,
    value_cache,
    valid,
    attn_gain,
    mlp_gain,
    query_scale,
    w_qkv,
    w_out,
    w_up,
    w_down,
    head_hidden,
    final_layer_matrices,
):
    rows, _, width = context_key_cache.shape
    heads = width // HD
    piece = np.arange(PIECE)
    y, core, mp = (lax.axis_index(axis) for axis in ("y", "c", "mp"))
    local = padded_rows(
        [head_hidden, jnp.transpose(final_layer_matrices, (0, 2, 1)).reshape(2 * PIECE, width)]
    )
    pairs = [(2 * a + m, 2 * ((a + NY // 2) % NY) + 1 - m) for a in range(NY) for m in range(2)]
    got = lax.ppermute(local, ("y", "mp"), pairs)
    keep = (y < NY // 2) == (mp == 0)
    finals = jnp.where(keep, local[PIECE : 3 * PIECE], got[PIECE : 3 * PIECE])
    second = padded_rows([local[:PIECE], got[:PIECE], finals])
    first = padded_rows(
        [jnp.transpose(w_qkv, (1, 0, 2)).reshape(3 * PIECE, width), w_out.T, w_up, w_down.T]
    )
    places = np.stack([piece * 3 + b for b in range(3)] + [piece + PIECE * b for b in range(3, 6)])
    shared = from_all(first, ("zh", "x")).reshape(-1, width)
    shared2 = from_all(second, "y").reshape(-1, width)
    block1 = dot(row_pick(places, NEAR, first.shape[0]), shared).astype(BF16)
    order = jnp.asarray(feature_order())
    all1 = lax.all_gather(block1, ("y", "c"), axis=0)
    _, shared2, new_embed, order = lax.optimization_barrier(
        (block1, shared2, new_embed, order)
    )
    shared2 = from_all(shared2, "zh").reshape(-1, width)
    pick = one_hot(output_rows(second.shape[0]), shared2.shape[0])
    block2 = dot(pick, shared2).astype(BF16)

    half = jnp.asarray(half_order())
    order2 = jnp.concatenate([half + PIECE * core, half + PIECE * (1 - core)])
    outs = jnp.asarray(output_order())
    outs = jnp.concatenate([outs + PIECE * core, outs + PIECE * (1 - core)])
    ids = jnp.arange(D, dtype=jnp.int32)
    forth = (ids[:, None] == order[None, :]).astype(BF16)
    turn = (order[:, None] == order2[None, :]).astype(BF16)
    plain = (order[:, None] == ids[None, :]).astype(BF16)
    last = (outs[:, None] == ids[None, : D // 2]).astype(BF16)

    normed = rms_scale(new_embed.astype(F32), attn_gain).astype(BF16)
    both = dot(jnp.concatenate([normed, new_embed], axis=0), forth).astype(BF16)
    normed_o, stream_o = both[:rows], both[rows:]
    gain_o = mlp_gain.reshape(NY, NZ, NX, NC, PIECE).transpose(0, 3, 1, 2, 4).reshape(1, D)
    pool = (jnp.arange(width)[:, None] // HD == jnp.arange(128)[None, :]).astype(BF16)
    scale = jnp.tile(query_scale, heads).reshape(1, width)
    used = jnp.broadcast_to(valid[:, None], (rows, 128))
    is_first = jnp.broadcast_to((mp == 0).astype(F32), (1, width))
    normed_o, stream_o, gain_o, pool, scale, used, is_first, turn, plain, last, block2 = (
        lax.optimization_barrier(
            (normed_o, stream_o, gain_o, pool, scale, used, is_first, turn, plain, last, block2)
        )
    )
    near = from_all(block2, "x")
    far = lax.ppermute(near, "c", [(0, 1), (1, 0)])

    part1 = attention_kernel(
        normed_o, scale, used, pool, context_key_cache, value_cache, all1
    )
    other1 = swap(part1)
    part2 = mlp_kernel(stream_o, part1, other1, gain_o, all1)
    other2 = swap(part2)
    return head_kernel(
        stream_o, part1, other1, part2, other2, is_first, turn, plain, last, near, far
    )


def solution(mesh):
    split = Mesh(
        mesh.devices.reshape(NY, NZ, NX, NC, mesh.shape["mp"]), ("y", "zh", "x", "c", "mp")
    )

    return jax.shard_map(
        per_device,
        mesh=split,
        in_specs=(
            P(DP, None),
            P(DP, None, "mp"),
            P(DP, None, "mp"),
            P(DP),
            P(),
            P(),
            P(),
            P(None, DP, "mp"),
            P("mp", DP),
            P(DP, "mp"),
            P("mp", DP),
            P(DP, "mp"),
            P(None, "mp", DP),
        ),
        out_specs=P(DP, "mp"),
        check_vma=False,
    )
```

```python
import math

import jax
import jax.numpy as jnp
import numpy as np
from jax import lax
from jax.experimental import pallas as pl
from jax.experimental.pallas import tpu as pltpu
from jax.sharding import Mesh
from jax.sharding import PartitionSpec as P

D = 1280
HEADS = 16
HD = D // HEADS
DP = ("y", "zh", "x", "c")
NY, NZ, NX, NC = 8, 4, 4, 2
PIECE = 5
NEAR = NZ * NX
BLK = NEAR * PIECE
FAR = NY * NC
STEP = 56
F32 = jnp.float32
BF16 = jnp.bfloat16


def feature_order():
    f = np.arange(D).reshape(NY, NZ, NX, NC, PIECE)
    return f.transpose(0, 3, 1, 2, 4).reshape(D).astype(np.int32)


def half_order():
    f = np.arange(D).reshape(NY, NZ, NX, NC, PIECE)[:, :, :, 0]
    return f.transpose(2, 1, 0, 3).reshape(D // NC).astype(np.int32)


def output_order():
    f = np.arange(D // 2).reshape(NY // 2, NZ, NX, NC, PIECE)[:, :, :, 0]
    return f.transpose(2, 1, 0, 3).reshape(D // 2 // NC).astype(np.int32)


def output_rows(padded):
    zh, y, piece = np.meshgrid(np.arange(NZ), np.arange(NY), np.arange(PIECE), indexing="ij")

    def at(slot, row):
        return (zh * NY + slot) * padded + row + piece

    def halves(row):
        src = at(y, row)
        return np.concatenate([src[:, : NY // 2].reshape(-1), src[:, NY // 2 :].reshape(-1)])

    own = at(y, 0).reshape(-1)
    other = at((y + NY // 2) % NY, PIECE).reshape(-1)
    return np.concatenate([own, other, halves(2 * PIECE), halves(3 * PIECE)])


def matrix_rows(places, padded):
    zh, x = np.meshgrid(np.arange(NZ), np.arange(NX), indexing="ij")
    device = (x * NZ + zh).reshape(-1)
    return (device[None, :, None] * padded + places[:, None, :]).reshape(-1)


def one_hot(src, count):
    src = jnp.asarray(src.astype(np.int32))
    return (src[:, None] == jnp.arange(count, dtype=jnp.int32)[None, :]).astype(BF16)


def padded_rows(parts):
    rows = jnp.concatenate(parts, axis=0)
    return jnp.pad(rows, ((0, -rows.shape[0] % 8), (0, 0)))


def from_all(array, axis):
    copies = jnp.broadcast_to(array, (lax.axis_size(axis), *array.shape))
    return lax.all_to_all(copies, axis, split_axis=0, concat_axis=0, tiled=True)


def in_hbm(array):
    return pltpu.with_memory_space_constraint(array, pltpu.HBM)


def in_vmem(array):
    return pltpu.with_memory_space_constraint(array, pltpu.VMEM)


def dot(a, b):
    return jnp.dot(a, b, preferred_element_type=F32)


def dot_t(a, b):
    return lax.dot_general(a, b, (((1,), (1,)), ((), ())), preferred_element_type=F32)


def attention_body(
    x_ref, scale_ref, valid_ref, pool_ref, k_ref, vals_hbm, w_hbm, out_ref, next_ref,
    w_buf, v_buf, q_buf, kn_buf, vn_buf, ctx_buf, sems,
):
    rows, width = q_buf.shape
    ctx_len = k_ref.shape[1]
    loads = [
        pltpu.make_async_copy(w_hbm.at[:, pl.ds(b * BLK, BLK), :], w_buf.at[b], sems.at[b])
        for b in range(4)
    ]
    later = [
        pltpu.make_async_copy(
            w_hbm.at[:, pl.ds((4 + b) * BLK, BLK), :], next_ref.at[b], sems.at[4 + b]
        )
        for b in range(2)
    ]
    load_v = pltpu.make_async_copy(vals_hbm, v_buf, sems.at[6])
    loads[0].start()
    loads[1].start()
    x = x_ref[...]
    loads[0].wait()
    loads[2].start()
    load_v.start()
    q = dot(x, w_buf[0].reshape(D, width))
    q_buf[...] = (q * scale_ref[...] / math.sqrt(HD)).astype(BF16).astype(F32)
    loads[1].wait()
    loads[3].start()
    for load in later:
        load.start()
    kn_buf[...] = dot(x, w_buf[1].reshape(D, width)).astype(BF16).astype(F32)
    loads[2].wait()
    vn_buf[...] = dot(x, w_buf[2].reshape(D, width)).astype(BF16).astype(F32)
    load_v.wait()
    pool = pool_ref[...]
    step = STEP

    def head_sums(prod):
        high = prod.astype(BF16)
        low = (prod - high.astype(F32)).astype(BF16)
        return dot(high, pool) + dot(low, pool)

    def body(i, carry):
        at = pl.multiple_of(i * step, 8)
        q8 = q_buf[pl.ds(at, step), :]
        k8 = k_ref[pl.ds(at, step)].astype(F32)
        prod = (q8[:, None, :] * k8).reshape(step * ctx_len, width)
        scores = head_sums(prod).reshape(step, ctx_len, 128)
        own = head_sums(q8 * kn_buf[pl.ds(at, step), :])
        used = valid_ref[pl.ds(at, step), :][:, None, :]
        slot = lax.broadcasted_iota(jnp.int32, (step, ctx_len, 128), 1)
        scores = jnp.where(slot < used, scores, -jnp.inf)
        top = jnp.maximum(jnp.max(scores, axis=1), own)
        e_cache = jnp.exp(scores - top[:, None, :])
        e_own = jnp.exp(own - top)
        total = jnp.sum(e_cache, axis=1) + e_own
        w_cache = (e_cache / total[:, None, :]).astype(BF16).reshape(step * ctx_len, 128)
        w_own = (e_own / total).astype(BF16)
        wide = dot_t(w_cache, pool).reshape(step, ctx_len, width)
        v8 = v_buf[pl.ds(at, step)].astype(F32)
        ctx = jnp.sum(wide * v8, axis=1)
        ctx_buf[pl.ds(at, step), :] = ctx + dot_t(w_own, pool) * vn_buf[pl.ds(at, step), :]
        return carry

    lax.fori_loop(0, rows // step, body, 0)
    loads[3].wait()
    out_ref[...] = dot_t(ctx_buf[...].astype(BF16), w_buf[3].reshape(D, width)).astype(BF16)
    for load in later:
        load.wait()


def attention_kernel(x, scale, valid, pool, keys, vals, w):
    rows, ctx_len, width = keys.shape
    vmem = pl.BlockSpec(memory_space=pltpu.VMEM)
    hbm = pl.BlockSpec(memory_space=pltpu.HBM)
    return pl.pallas_call(
        attention_body,
        out_shape=(pltpu.VMEM((rows, D), BF16), pltpu.VMEM((2, FAR, BLK, width), BF16)),
        in_specs=[vmem] * 5 + [hbm] * 2,
        out_specs=(vmem, vmem),
        scratch_shapes=[
            pltpu.VMEM((4, FAR, BLK, width), BF16),
            pltpu.VMEM((rows, ctx_len, width), BF16),
            pltpu.VMEM((rows, width), F32),
            pltpu.VMEM((rows, width), F32),
            pltpu.VMEM((rows, width), F32),
            pltpu.VMEM((rows, width), F32),
            pltpu.SemaphoreType.DMA((7,)),
        ],
        compiler_params=pltpu.CompilerParams(vmem_limit_bytes=36 * 2**20),
        name="attend",
    )(x, scale, valid, pool, in_vmem(keys), in_hbm(vals), in_hbm(w))


def mlp_body(stream_ref, own_ref, other_ref, gain_ref, w_ref, out_ref):
    width = w_ref.shape[-1]
    s1 = stream_ref[...].astype(F32) + (own_ref[...].astype(F32) + other_ref[...].astype(F32))
    meansq = jnp.mean(s1 * s1, axis=-1, keepdims=True)
    n2 = (s1 * lax.rsqrt(meansq + 1e-06) * gain_ref[...]).astype(BF16)
    hidden = jnp.maximum(dot(n2, w_ref[0].reshape(D, width)), 0.0).astype(BF16)
    out_ref[...] = dot_t(hidden, w_ref[1].reshape(D, width)).astype(BF16)


def mlp_kernel(stream, own, other, gain, w):
    rows = stream.shape[0]
    vmem = pl.BlockSpec(memory_space=pltpu.VMEM)
    return pl.pallas_call(
        mlp_body,
        out_shape=pltpu.VMEM((rows, D), BF16),
        in_specs=[vmem] * 5,
        out_specs=vmem,
        compiler_params=pltpu.CompilerParams(vmem_limit_bytes=12 * 2**20),
        name="mlp",
    )(stream, own, other, gain, in_vmem(w))


def head_body(
    stream_ref, own1_ref, other1_ref, own2_ref, other2_ref, first_ref, far_ref,
    turn_hbm, plain_hbm, last_hbm, near_hbm,
    out_ref, turn_buf, plain_buf, last_buf, near_ref, sems,
):
    width = near_ref.shape[-1]
    half = D // NC
    each = half // NX
    rows = 2 * each
    load_turn = pltpu.make_async_copy(turn_hbm, turn_buf, sems.at[0])
    load_plain = pltpu.make_async_copy(plain_hbm, plain_buf, sems.at[1])
    load_last = pltpu.make_async_copy(last_hbm, last_buf, sems.at[2])
    loads = [
        pltpu.make_async_copy(
            near_hbm.at[:, pl.ds(n * rows, rows), :],
            near_ref.at[:, pl.ds(n * rows, rows), :],
            sems.at[3 + n],
        )
        for n in range(2)
    ]
    load_turn.start()
    loads[0].start()

    def part(ref, start, count):
        return ref[:, pl.ds(start, count), :].reshape(NX * count, width)

    s1 = stream_ref[...].astype(F32) + (own1_ref[...].astype(F32) + other1_ref[...].astype(F32))
    s2 = (s1 + (own2_ref[...].astype(F32) + other2_ref[...].astype(F32))).astype(BF16)
    load_turn.wait()
    load_plain.start()
    loads[1].start()
    load_last.start()
    turned = dot(s2, turn_buf[...]).astype(BF16)
    loads[0].wait()

    def hidden(start):
        pre = dot(turned[:, :half], part(near_ref, start, each))
        pre = pre + dot(turned[:, half:], part(far_ref, start, each))
        return (pre / (1.0 + jnp.exp(-pre))).astype(BF16)

    act_own = hidden(0)
    act_other = hidden(each)
    first = first_ref[...] > 0
    act = (jnp.where(first, act_own, act_other), jnp.where(first, act_other, act_own))
    load_plain.wait()
    plain = dot(s2, plain_buf[...]).astype(BF16)
    skip = (plain[:, :width], plain[:, width:])
    loads[1].wait()
    out = []
    for ref in (near_ref, far_ref):
        total = None
        for k in range(2):
            at = 2 * each + k * (each // 2)
            term = dot_t(act[k], part(ref, at, each // 2))
            term = term + dot_t(skip[k], part(ref, at + each, each // 2))
            total = term if total is None else total + term
        out.append(total)
    out = jnp.concatenate(out, axis=1)
    high = out.astype(BF16)
    low = (out - high.astype(F32)).astype(BF16)
    load_last.wait()
    out_ref[...] = dot(high, last_buf[...]) + dot(low, last_buf[...])


def head_kernel(stream, own1, other1, own2, other2, first, turn, plain, last, near, far):
    rows = stream.shape[0]
    width = near.shape[-1]
    vmem = pl.BlockSpec(memory_space=pltpu.VMEM)
    hbm = pl.BlockSpec(memory_space=pltpu.HBM)
    return pl.pallas_call(
        head_body,
        out_shape=jax.ShapeDtypeStruct((rows, width), F32),
        in_specs=[vmem] * 7 + [hbm] * 4,
        out_specs=vmem,
        scratch_shapes=[
            pltpu.VMEM(turn.shape, BF16),
            pltpu.VMEM(plain.shape, BF16),
            pltpu.VMEM(last.shape, BF16),
            pltpu.VMEM(near.shape, BF16),
            pltpu.SemaphoreType.DMA((5,)),
        ],
        compiler_params=pltpu.CompilerParams(vmem_limit_bytes=32 * 2**20),
        name="head",
    )(
        stream, own1, other1, own2, other2, first, in_vmem(far),
        in_hbm(turn), in_hbm(plain), in_hbm(last), in_hbm(near),
    )


def rms_scale(values, gain):
    meansq = jnp.mean(values * values, axis=-1, keepdims=True)
    return values * lax.rsqrt(meansq + 1e-06) * gain


def swap(array):
    return lax.ppermute(array, "mp", [(0, 1), (1, 0)])


def per_device(
    new_embed,
    context_key_cache,
    value_cache,
    valid,
    attn_gain,
    mlp_gain,
    query_scale,
    w_qkv,
    w_out,
    w_up,
    w_down,
    head_hidden,
    final_layer_matrices,
):
    rows, _, width = context_key_cache.shape
    heads = width // HD
    piece = np.arange(PIECE)
    y, core, mp = (lax.axis_index(axis) for axis in ("y", "c", "mp"))
    local = padded_rows(
        [head_hidden, jnp.transpose(final_layer_matrices, (0, 2, 1)).reshape(2 * PIECE, width)]
    )
    pairs = [(2 * a + m, 2 * ((a + NY // 2) % NY) + 1 - m) for a in range(NY) for m in range(2)]
    got = lax.ppermute(local, ("y", "mp"), pairs)
    keep = (y < NY // 2) == (mp == 0)
    finals = jnp.where(keep, local[PIECE : 3 * PIECE], got[PIECE : 3 * PIECE])
    second = padded_rows([local[:PIECE], got[:PIECE], finals])
    first = padded_rows(
        [jnp.transpose(w_qkv, (1, 0, 2)).reshape(3 * PIECE, width), w_out.T, w_up, w_down.T]
    )
    places = np.stack([piece * 3 + b for b in range(3)] + [piece + PIECE * b for b in range(3, 6)])
    shared = from_all(first, "zh").reshape(-1, width)
    shared = from_all(shared, "x").reshape(-1, width)
    shared2 = from_all(second, "y").reshape(-1, width)
    pick = one_hot(matrix_rows(places, first.shape[0]), shared.shape[0])
    block1 = dot(pick, shared).astype(BF16)
    order = jnp.asarray(feature_order())
    all1 = lax.all_gather(block1, ("y", "c"), axis=0)
    _, shared2, new_embed, order = lax.optimization_barrier(
        (block1, shared2, new_embed, order)
    )
    shared2 = from_all(shared2, "zh").reshape(-1, width)
    pick = one_hot(output_rows(second.shape[0]), shared2.shape[0])
    block2 = dot(pick, shared2).astype(BF16)

    half = jnp.asarray(half_order())
    order2 = jnp.concatenate([half + PIECE * core, half + PIECE * (1 - core)])
    outs = jnp.asarray(output_order())
    outs = jnp.concatenate([outs + PIECE * core, outs + PIECE * (1 - core)])
    ids = jnp.arange(D, dtype=jnp.int32)
    forth = (ids[:, None] == order[None, :]).astype(BF16)
    turn = (order[:, None] == order2[None, :]).astype(BF16)
    plain = (order[:, None] == ids[None, :]).astype(BF16)
    last = (outs[:, None] == ids[None, : D // 2]).astype(BF16)

    normed = rms_scale(new_embed.astype(F32), attn_gain).astype(BF16)
    both = dot(jnp.concatenate([normed, new_embed], axis=0), forth).astype(BF16)
    normed_o, stream_o = both[:rows], both[rows:]
    gain_o = mlp_gain.reshape(NY, NZ, NX, NC, PIECE).transpose(0, 3, 1, 2, 4).reshape(1, D)
    pool = (jnp.arange(width)[:, None] // HD == jnp.arange(128)[None, :]).astype(BF16)
    scale = jnp.tile(query_scale, heads).reshape(1, width)
    used = jnp.broadcast_to(valid[:, None], (rows, 128))
    is_first = jnp.broadcast_to((mp == 0).astype(F32), (1, width))
    normed_o, stream_o, gain_o, pool, scale, used, is_first, turn, plain, last, block2 = (
        lax.optimization_barrier(
            (normed_o, stream_o, gain_o, pool, scale, used, is_first, turn, plain, last, block2)
        )
    )
    near = from_all(block2, "x")
    far = lax.ppermute(near, "c", [(0, 1), (1, 0)])

    part1, feed_w = attention_kernel(
        normed_o, scale, used, pool, context_key_cache, value_cache, all1
    )
    other1 = swap(part1)
    part2 = mlp_kernel(stream_o, part1, other1, gain_o, feed_w)
    other2 = swap(part2)
    return head_kernel(
        stream_o, part1, other1, part2, other2, is_first, turn, plain, last, near, far
    )


def solution(mesh):
    split = Mesh(
        mesh.devices.reshape(NY, NZ, NX, NC, mesh.shape["mp"]), ("y", "zh", "x", "c", "mp")
    )

    return jax.shard_map(
        per_device,
        mesh=split,
        in_specs=(
            P(DP, None),
            P(DP, None, "mp"),
            P(DP, None, "mp"),
            P(DP),
            P(),
            P(),
            P(),
            P(None, DP, "mp"),
            P("mp", DP),
            P(DP, "mp"),
            P("mp", DP),
            P(DP, "mp"),
            P(None, "mp", DP),
        ),
        out_specs=P(DP, "mp"),
        check_vma=False,
    )
```

```python
import math

import jax
import jax.numpy as jnp
import numpy as np
from jax import lax
from jax.experimental import pallas as pl
from jax.experimental.pallas import tpu as pltpu
from jax.sharding import Mesh
from jax.sharding import PartitionSpec as P

D = 1280
HEADS = 16
HD = D // HEADS
DP = ("y", "zh", "x", "c")
NY, NZ, NX, NC = 8, 4, 4, 2
PIECE = 5
NEAR = NZ * NX
BLK = NEAR * PIECE
FAR = NY * NC
STEP = 56
F32 = jnp.float32
BF16 = jnp.bfloat16


def feature_order():
    f = np.arange(D).reshape(NY, NZ, NX, NC, PIECE)
    return f.transpose(0, 3, 1, 2, 4).reshape(D).astype(np.int32)


def half_order():
    f = np.arange(D).reshape(NY, NZ, NX, NC, PIECE)[:, :, :, 0]
    return f.transpose(2, 1, 0, 3).reshape(D // NC).astype(np.int32)


def output_order():
    f = np.arange(D // 2).reshape(NY // 2, NZ, NX, NC, PIECE)[:, :, :, 0]
    return f.transpose(2, 1, 0, 3).reshape(D // 2 // NC).astype(np.int32)


def first_rows(padded):
    y, piece = np.meshgrid(np.arange(NY), np.arange(PIECE), indexing="ij")

    def hidden(half):
        return ((y * 2 + half) * padded + piece).reshape(-1)

    def final(k):
        lower = y[: NY // 2], piece[: NY // 2]
        return np.concatenate(
            [((lower[0] * 2 + half) * padded + k * PIECE + lower[1]).reshape(-1) for half in range(2)]
        )

    rows = np.concatenate([hidden(0), hidden(1), final(1), final(2)])
    step = np.repeat([0, NY * padded], NY * 2 * PIECE)
    return rows.astype(np.int32), step.astype(np.int32)


def second_rows():
    each = NY * PIECE
    zh = np.arange(NZ)[:, None]

    def block(start, count):
        return (zh * 4 * each + start + np.arange(count)[None, :]).reshape(-1)

    whole = [block(n * each, each) for n in range(2)]
    halves = [block(n * (each // 2), each // 2) for n in range(4, 8)]
    return np.concatenate(whole + halves)


def matrix_rows(places, padded):
    zh, x = np.meshgrid(np.arange(NZ), np.arange(NX), indexing="ij")
    device = (x * NZ + zh).reshape(-1)
    return (device[None, :, None] * padded + places[:, None, :]).reshape(-1)


def one_hot(src, count):
    src = jnp.asarray(src, jnp.int32)
    return (src[:, None] == jnp.arange(count, dtype=jnp.int32)[None, :]).astype(BF16)


def padded_rows(parts):
    rows = jnp.concatenate(parts, axis=0)
    return jnp.pad(rows, ((0, -rows.shape[0] % 8), (0, 0)))


def from_all(array, axis):
    copies = jnp.broadcast_to(array, (lax.axis_size(axis), *array.shape))
    return lax.all_to_all(copies, axis, split_axis=0, concat_axis=0, tiled=True)


def in_hbm(array):
    return pltpu.with_memory_space_constraint(array, pltpu.HBM)


def in_vmem(array):
    return pltpu.with_memory_space_constraint(array, pltpu.VMEM)


def dot(a, b):
    return jnp.dot(a, b, preferred_element_type=F32)


def dot_t(a, b):
    return lax.dot_general(a, b, (((1,), (1,)), ((), ())), preferred_element_type=F32)


def attention_body(
    x_ref, scale_ref, valid_ref, pool_ref, k_ref, vals_hbm, w_hbm, out_ref, next_ref,
    w_buf, v_buf, q_buf, kn_buf, vn_buf, ctx_buf, sems,
):
    rows, width = q_buf.shape
    ctx_len = k_ref.shape[1]
    loads = [
        pltpu.make_async_copy(w_hbm.at[:, pl.ds(b * BLK, BLK), :], w_buf.at[b], sems.at[b])
        for b in range(4)
    ]
    later = [
        pltpu.make_async_copy(
            w_hbm.at[:, pl.ds((4 + b) * BLK, BLK), :], next_ref.at[b], sems.at[4 + b]
        )
        for b in range(2)
    ]
    load_v = pltpu.make_async_copy(vals_hbm, v_buf, sems.at[6])
    loads[0].start()
    loads[1].start()
    x = x_ref[...]
    loads[0].wait()
    loads[2].start()
    load_v.start()
    q = dot(x, w_buf[0].reshape(D, width))
    q_buf[...] = (q * scale_ref[...] / math.sqrt(HD)).astype(BF16).astype(F32)
    loads[1].wait()
    loads[3].start()
    for load in later:
        load.start()
    kn_buf[...] = dot(x, w_buf[1].reshape(D, width)).astype(BF16).astype(F32)
    loads[2].wait()
    vn_buf[...] = dot(x, w_buf[2].reshape(D, width)).astype(BF16).astype(F32)
    load_v.wait()
    pool = pool_ref[...]
    step = STEP

    def head_sums(prod):
        high = prod.astype(BF16)
        low = (prod - high.astype(F32)).astype(BF16)
        return dot(high, pool) + dot(low, pool)

    def body(i, carry):
        at = pl.multiple_of(i * step, 8)
        q8 = q_buf[pl.ds(at, step), :]
        k8 = k_ref[pl.ds(at, step)].astype(F32)
        prod = (q8[:, None, :] * k8).reshape(step * ctx_len, width)
        scores = head_sums(prod).reshape(step, ctx_len, 128)
        own = head_sums(q8 * kn_buf[pl.ds(at, step), :])
        used = valid_ref[pl.ds(at, step), :][:, None, :]
        slot = lax.broadcasted_iota(jnp.int32, (step, ctx_len, 128), 1)
        scores = jnp.where(slot < used, scores, -jnp.inf)
        top = jnp.maximum(jnp.max(scores, axis=1), own)
        e_cache = jnp.exp(scores - top[:, None, :])
        e_own = jnp.exp(own - top)
        total = jnp.sum(e_cache, axis=1) + e_own
        w_cache = (e_cache / total[:, None, :]).astype(BF16).reshape(step * ctx_len, 128)
        w_own = (e_own / total).astype(BF16)
        wide = dot_t(w_cache, pool).reshape(step, ctx_len, width)
        v8 = v_buf[pl.ds(at, step)].astype(F32)
        ctx = jnp.sum(wide * v8, axis=1)
        ctx_buf[pl.ds(at, step), :] = ctx + dot_t(w_own, pool) * vn_buf[pl.ds(at, step), :]
        return carry

    lax.fori_loop(0, rows // step, body, 0)
    loads[3].wait()
    out_ref[...] = dot_t(ctx_buf[...].astype(BF16), w_buf[3].reshape(D, width)).astype(BF16)
    for load in later:
        load.wait()


def attention_kernel(x, scale, valid, pool, keys, vals, w):
    rows, ctx_len, width = keys.shape
    vmem = pl.BlockSpec(memory_space=pltpu.VMEM)
    hbm = pl.BlockSpec(memory_space=pltpu.HBM)
    return pl.pallas_call(
        attention_body,
        out_shape=(pltpu.VMEM((rows, D), BF16), pltpu.VMEM((2, FAR, BLK, width), BF16)),
        in_specs=[vmem] * 5 + [hbm] * 2,
        out_specs=(vmem, vmem),
        scratch_shapes=[
            pltpu.VMEM((4, FAR, BLK, width), BF16),
            pltpu.VMEM((rows, ctx_len, width), BF16),
            pltpu.VMEM((rows, width), F32),
            pltpu.VMEM((rows, width), F32),
            pltpu.VMEM((rows, width), F32),
            pltpu.VMEM((rows, width), F32),
            pltpu.SemaphoreType.DMA((7,)),
        ],
        compiler_params=pltpu.CompilerParams(vmem_limit_bytes=36 * 2**20),
        name="attend",
    )(x, scale, valid, pool, in_vmem(keys), in_hbm(vals), in_hbm(w))


def mlp_body(stream_ref, own_ref, other_ref, gain_ref, w_ref, out_ref):
    width = w_ref.shape[-1]
    s1 = stream_ref[...].astype(F32) + (own_ref[...].astype(F32) + other_ref[...].astype(F32))
    meansq = jnp.mean(s1 * s1, axis=-1, keepdims=True)
    n2 = (s1 * lax.rsqrt(meansq + 1e-06) * gain_ref[...]).astype(BF16)
    hidden = jnp.maximum(dot(n2, w_ref[0].reshape(D, width)), 0.0).astype(BF16)
    out_ref[...] = dot_t(hidden, w_ref[1].reshape(D, width)).astype(BF16)


def mlp_kernel(stream, own, other, gain, w):
    rows = stream.shape[0]
    vmem = pl.BlockSpec(memory_space=pltpu.VMEM)
    return pl.pallas_call(
        mlp_body,
        out_shape=pltpu.VMEM((rows, D), BF16),
        in_specs=[vmem] * 5,
        out_specs=vmem,
        compiler_params=pltpu.CompilerParams(vmem_limit_bytes=12 * 2**20),
        name="mlp",
    )(stream, own, other, gain, in_vmem(w))


def head_body(
    stream_ref, own1_ref, other1_ref, own2_ref, other2_ref, far_ref,
    turn_hbm, plain_hbm, last_hbm, near_hbm,
    out_ref, turn_buf, plain_buf, last_buf, near_ref, sems,
):
    width = near_ref.shape[-1]
    half = D // NC
    each = half // NX
    rows = 2 * each
    load_turn = pltpu.make_async_copy(turn_hbm, turn_buf, sems.at[0])
    load_plain = pltpu.make_async_copy(plain_hbm, plain_buf, sems.at[1])
    load_last = pltpu.make_async_copy(last_hbm, last_buf, sems.at[2])
    loads = [
        pltpu.make_async_copy(
            near_hbm.at[:, pl.ds(n * rows, rows), :],
            near_ref.at[:, pl.ds(n * rows, rows), :],
            sems.at[3 + n],
        )
        for n in range(2)
    ]
    load_turn.start()
    loads[0].start()

    def part(ref, start, count):
        return ref[:, pl.ds(start, count), :].reshape(NX * count, width)

    s1 = stream_ref[...].astype(F32) + (own1_ref[...].astype(F32) + other1_ref[...].astype(F32))
    s2 = (s1 + (own2_ref[...].astype(F32) + other2_ref[...].astype(F32))).astype(BF16)
    load_turn.wait()
    load_plain.start()
    loads[1].start()
    load_last.start()
    turned = dot(s2, turn_buf[...]).astype(BF16)
    loads[0].wait()

    def hidden(start):
        pre = dot(turned[:, :half], part(near_ref, start, each))
        pre = pre + dot(turned[:, half:], part(far_ref, start, each))
        return (pre / (1.0 + jnp.exp(-pre))).astype(BF16)

    act = (hidden(0), hidden(each))
    load_plain.wait()
    plain = dot(s2, plain_buf[...]).astype(BF16)
    skip = (plain[:, :width], plain[:, width:])
    loads[1].wait()
    out = []
    for ref in (near_ref, far_ref):
        total = None
        for k in range(2):
            at = 2 * each + k * (each // 2)
            term = dot_t(act[k], part(ref, at, each // 2))
            term = term + dot_t(skip[k], part(ref, at + each, each // 2))
            total = term if total is None else total + term
        out.append(total)
    out = jnp.concatenate(out, axis=1)
    high = out.astype(BF16)
    low = (out - high.astype(F32)).astype(BF16)
    load_last.wait()
    out_ref[...] = dot(high, last_buf[...]) + dot(low, last_buf[...])


def head_kernel(stream, own1, other1, own2, other2, turn, plain, last, near, far):
    rows = stream.shape[0]
    width = near.shape[-1]
    vmem = pl.BlockSpec(memory_space=pltpu.VMEM)
    hbm = pl.BlockSpec(memory_space=pltpu.HBM)
    return pl.pallas_call(
        head_body,
        out_shape=jax.ShapeDtypeStruct((rows, width), F32),
        in_specs=[vmem] * 6 + [hbm] * 4,
        out_specs=vmem,
        scratch_shapes=[
            pltpu.VMEM(turn.shape, BF16),
            pltpu.VMEM(plain.shape, BF16),
            pltpu.VMEM(last.shape, BF16),
            pltpu.VMEM(near.shape, BF16),
            pltpu.SemaphoreType.DMA((5,)),
        ],
        compiler_params=pltpu.CompilerParams(vmem_limit_bytes=32 * 2**20),
        name="head",
    )(
        stream, own1, other1, own2, other2, in_vmem(far),
        in_hbm(turn), in_hbm(plain), in_hbm(last), in_hbm(near),
    )


def rms_scale(values, gain):
    meansq = jnp.mean(values * values, axis=-1, keepdims=True)
    return values * lax.rsqrt(meansq + 1e-06) * gain


def swap(array):
    return lax.ppermute(array, "mp", [(0, 1), (1, 0)])


def per_device(
    new_embed,
    context_key_cache,
    value_cache,
    valid,
    attn_gain,
    mlp_gain,
    query_scale,
    w_qkv,
    w_out,
    w_up,
    w_down,
    head_hidden,
    final_layer_matrices,
):
    rows, _, width = context_key_cache.shape
    heads = width // HD
    piece = np.arange(PIECE)
    core, mp = lax.axis_index("c"), lax.axis_index("mp")
    second = padded_rows(
        [head_hidden, jnp.transpose(final_layer_matrices, (0, 2, 1)).reshape(2 * PIECE, width)]
    )
    first = padded_rows(
        [jnp.transpose(w_qkv, (1, 0, 2)).reshape(3 * PIECE, width), w_out.T, w_up, w_down.T]
    )
    places = np.stack([piece * 3 + b for b in range(3)] + [piece + PIECE * b for b in range(3, 6)])
    shared = from_all(first, "zh").reshape(-1, width)
    shared = from_all(shared, "x").reshape(-1, width)
    shared2 = from_all(second, ("y", "mp")).reshape(-1, width)
    pick = one_hot(matrix_rows(places, first.shape[0]), shared.shape[0])
    block1 = dot(pick, shared).astype(BF16)
    order = jnp.asarray(feature_order())
    all1 = lax.all_gather(block1, ("y", "c"), axis=0)
    _, shared2, new_embed, order = lax.optimization_barrier(
        (block1, shared2, new_embed, order)
    )
    src, step = first_rows(second.shape[0])
    pick = one_hot(jnp.asarray(src) + jnp.asarray(step) * mp, shared2.shape[0])
    shared2 = dot(pick, shared2).astype(BF16)
    shared2 = from_all(shared2, "zh").reshape(-1, width)
    block2 = dot(one_hot(second_rows(), shared2.shape[0]), shared2).astype(BF16)

    half = jnp.asarray(half_order())
    order2 = jnp.concatenate([half + PIECE * core, half + PIECE * (1 - core)])
    outs = jnp.asarray(output_order())
    outs = jnp.concatenate([outs + PIECE * core, outs + PIECE * (1 - core)])
    ids = jnp.arange(D, dtype=jnp.int32)
    forth = (ids[:, None] == order[None, :]).astype(BF16)
    turn = (order[:, None] == order2[None, :]).astype(BF16)
    plain = (order[:, None] == ids[None, :]).astype(BF16)
    last = (outs[:, None] == ids[None, : D // 2]).astype(BF16)

    normed = rms_scale(new_embed.astype(F32), attn_gain).astype(BF16)
    both = dot(jnp.concatenate([normed, new_embed], axis=0), forth).astype(BF16)
    normed_o, stream_o = both[:rows], both[rows:]
    gain_o = mlp_gain.reshape(NY, NZ, NX, NC, PIECE).transpose(0, 3, 1, 2, 4).reshape(1, D)
    pool = (jnp.arange(width)[:, None] // HD == jnp.arange(128)[None, :]).astype(BF16)
    scale = jnp.tile(query_scale, heads).reshape(1, width)
    used = jnp.broadcast_to(valid[:, None], (rows, 128))
    normed_o, stream_o, gain_o, pool, scale, used, turn, plain, last, block2 = (
        lax.optimization_barrier(
            (normed_o, stream_o, gain_o, pool, scale, used, turn, plain, last, block2)
        )
    )
    near = from_all(block2, "x")
    far = lax.ppermute(near, "c", [(0, 1), (1, 0)])

    part1, feed_w = attention_kernel(
        normed_o, scale, used, pool, context_key_cache, value_cache, all1
    )
    other1 = swap(part1)
    part2 = mlp_kernel(stream_o, part1, other1, gain_o, feed_w)
    other2 = swap(part2)
    return head_kernel(
        stream_o, part1, other1, part2, other2, turn, plain, last, near, far
    )


def solution(mesh):
    split = Mesh(
        mesh.devices.reshape(NY, NZ, NX, NC, mesh.shape["mp"]), ("y", "zh", "x", "c", "mp")
    )

    return jax.shard_map(
        per_device,
        mesh=split,
        in_specs=(
            P(DP, None),
            P(DP, None, "mp"),
            P(DP, None, "mp"),
            P(DP),
            P(),
            P(),
            P(),
            P(None, DP, "mp"),
            P("mp", DP),
            P(DP, "mp"),
            P("mp", DP),
            P(DP, "mp"),
            P(None, "mp", DP),
        ),
        out_specs=P(DP, "mp"),
        check_vma=False,
    )
```

```python
import math

import jax
import jax.numpy as jnp
import numpy as np
from jax import lax
from jax.experimental import pallas as pl
from jax.experimental.pallas import tpu as pltpu
from jax.sharding import Mesh
from jax.sharding import PartitionSpec as P

D = 1280
HEADS = 16
HD = D // HEADS
DP = ("y", "zh", "x", "c")
NY, NZ, NX, NC = 8, 4, 4, 2
PIECE = 5
NEAR = NZ * NX
BLK = NEAR * PIECE
FAR = NY * NC
STEP = 56
F32 = jnp.float32
BF16 = jnp.bfloat16


def feature_order():
    f = np.arange(D).reshape(NY, NZ, NX, NC, PIECE)
    return f.transpose(0, 3, 1, 2, 4).reshape(D).astype(np.int32)


def half_order():
    f = np.arange(D).reshape(NY, NZ, NX, NC, PIECE)[:, :, :, 0]
    return f.transpose(2, 1, 0, 3).reshape(D // NC).astype(np.int32)


def output_order():
    f = np.arange(D // 2).reshape(NY // 2, NZ, NX, NC, PIECE)[:, :, :, 0]
    return f.transpose(2, 1, 0, 3).reshape(D // 2 // NC).astype(np.int32)


def first_rows(padded):
    y, piece = np.meshgrid(np.arange(NY), np.arange(PIECE), indexing="ij")

    def hidden(half):
        return ((y * 2 + half) * padded + piece).reshape(-1)

    def final(k):
        lower = y[: NY // 2], piece[: NY // 2]
        return np.concatenate(
            [((lower[0] * 2 + half) * padded + k * PIECE + lower[1]).reshape(-1) for half in range(2)]
        )

    rows = np.concatenate([hidden(0), hidden(1), final(1), final(2)])
    step = np.repeat([0, NY * padded], NY * 2 * PIECE)
    return rows.astype(np.int32), step.astype(np.int32)


def second_rows():
    each = NY * PIECE
    zh = np.arange(NZ)[:, None]

    def block(start, count):
        return (zh * 4 * each + start + np.arange(count)[None, :]).reshape(-1)

    whole = [block(n * each, each) for n in range(2)]
    halves = [block(n * (each // 2), each // 2) for n in range(4, 8)]
    return np.concatenate(whole + halves)


def matrix_rows(places, padded):
    zh, x = np.meshgrid(np.arange(NZ), np.arange(NX), indexing="ij")
    device = (x * NZ + zh).reshape(-1)
    return (device[None, :, None] * padded + places[:, None, :]).reshape(-1)


def one_hot(src, count):
    src = jnp.asarray(src, jnp.int32)
    return (src[:, None] == jnp.arange(count, dtype=jnp.int32)[None, :]).astype(BF16)


def padded_rows(parts):
    rows = jnp.concatenate(parts, axis=0)
    return jnp.pad(rows, ((0, -rows.shape[0] % 8), (0, 0)))


def from_all(array, axis):
    copies = jnp.broadcast_to(array, (lax.axis_size(axis), *array.shape))
    return lax.all_to_all(copies, axis, split_axis=0, concat_axis=0, tiled=True)


def in_hbm(array):
    return pltpu.with_memory_space_constraint(array, pltpu.HBM)


def in_vmem(array):
    return pltpu.with_memory_space_constraint(array, pltpu.VMEM)


def dot(a, b):
    return jnp.dot(a, b, preferred_element_type=F32)


def dot_t(a, b):
    return lax.dot_general(a, b, (((1,), (1,)), ((), ())), preferred_element_type=F32)


def attention_body(
    x_ref, scale_ref, valid_ref, pool_ref, k_ref, vals_hbm, w_hbm, out_ref, next_ref,
    w_buf, v_buf, q_buf, kn_buf, vn_buf, ctx_buf, sems,
):
    rows, width = q_buf.shape
    ctx_len = k_ref.shape[1]
    loads = [
        pltpu.make_async_copy(w_hbm.at[:, pl.ds(b * BLK, BLK), :], w_buf.at[b], sems.at[b])
        for b in range(4)
    ]
    later = [
        pltpu.make_async_copy(
            w_hbm.at[:, pl.ds((4 + b) * BLK, BLK), :], next_ref.at[b], sems.at[4 + b]
        )
        for b in range(2)
    ]
    load_v = pltpu.make_async_copy(vals_hbm, v_buf, sems.at[6])
    loads[0].start()
    loads[1].start()
    x = x_ref[...]
    loads[0].wait()
    loads[2].start()
    load_v.start()
    q = dot(x, w_buf[0].reshape(D, width))
    q_buf[...] = (q * scale_ref[...] / math.sqrt(HD)).astype(BF16).astype(F32)
    loads[1].wait()
    loads[3].start()
    for load in later:
        load.start()
    kn_buf[...] = dot(x, w_buf[1].reshape(D, width)).astype(BF16).astype(F32)
    loads[2].wait()
    vn_buf[...] = dot(x, w_buf[2].reshape(D, width)).astype(BF16).astype(F32)
    load_v.wait()
    pool = pool_ref[...]
    step = STEP

    def head_sums(prod):
        high = prod.astype(BF16)
        low = (prod - high.astype(F32)).astype(BF16)
        return dot(high, pool) + dot(low, pool)

    def body(i, carry):
        at = pl.multiple_of(i * step, 8)
        q8 = q_buf[pl.ds(at, step), :]
        k8 = k_ref[pl.ds(at, step)].astype(F32)
        prod = (q8[:, None, :] * k8).reshape(step * ctx_len, width)
        scores = head_sums(prod).reshape(step, ctx_len, 128)
        own = head_sums(q8 * kn_buf[pl.ds(at, step), :])
        used = valid_ref[pl.ds(at, step), :][:, None, :]
        slot = lax.broadcasted_iota(jnp.int32, (step, ctx_len, 128), 1)
        scores = jnp.where(slot < used, scores, -jnp.inf)
        top = jnp.maximum(jnp.max(scores, axis=1), own)
        e_cache = jnp.exp(scores - top[:, None, :])
        e_own = jnp.exp(own - top)
        total = jnp.sum(e_cache, axis=1) + e_own
        w_cache = (e_cache / total[:, None, :]).astype(BF16).reshape(step * ctx_len, 128)
        w_own = (e_own / total).astype(BF16)
        wide = dot_t(w_cache, pool).reshape(step, ctx_len, width)
        v8 = v_buf[pl.ds(at, step)].astype(F32)
        ctx = jnp.sum(wide * v8, axis=1)
        ctx_buf[pl.ds(at, step), :] = ctx + dot_t(w_own, pool) * vn_buf[pl.ds(at, step), :]
        return carry

    lax.fori_loop(0, rows // step, body, 0)
    loads[3].wait()
    out_ref[...] = dot_t(ctx_buf[...].astype(BF16), w_buf[3].reshape(D, width)).astype(BF16)
    for load in later:
        load.wait()


def attention_kernel(x, scale, valid, pool, keys, vals, w):
    rows, ctx_len, width = keys.shape
    vmem = pl.BlockSpec(memory_space=pltpu.VMEM)
    hbm = pl.BlockSpec(memory_space=pltpu.HBM)
    return pl.pallas_call(
        attention_body,
        out_shape=(pltpu.VMEM((rows, D), BF16), pltpu.VMEM((2, FAR, BLK, width), BF16)),
        in_specs=[vmem] * 5 + [hbm] * 2,
        out_specs=(vmem, vmem),
        scratch_shapes=[
            pltpu.VMEM((4, FAR, BLK, width), BF16),
            pltpu.VMEM((rows, ctx_len, width), BF16),
            pltpu.VMEM((rows, width), F32),
            pltpu.VMEM((rows, width), F32),
            pltpu.VMEM((rows, width), F32),
            pltpu.VMEM((rows, width), F32),
            pltpu.SemaphoreType.DMA((7,)),
        ],
        compiler_params=pltpu.CompilerParams(vmem_limit_bytes=36 * 2**20),
        name="attend",
    )(x, scale, valid, pool, in_vmem(keys), in_hbm(vals), in_hbm(w))


def mlp_body(stream_ref, own_ref, other_ref, gain_ref, w_ref, out_ref):
    width = w_ref.shape[-1]
    s1 = stream_ref[...].astype(F32) + (own_ref[...].astype(F32) + other_ref[...].astype(F32))
    meansq = jnp.mean(s1 * s1, axis=-1, keepdims=True)
    n2 = (s1 * lax.rsqrt(meansq + 1e-06) * gain_ref[...]).astype(BF16)
    hidden = jnp.maximum(dot(n2, w_ref[0].reshape(D, width)), 0.0).astype(BF16)
    out_ref[...] = dot_t(hidden, w_ref[1].reshape(D, width)).astype(BF16)


def mlp_kernel(stream, own, other, gain, w):
    rows = stream.shape[0]
    vmem = pl.BlockSpec(memory_space=pltpu.VMEM)
    return pl.pallas_call(
        mlp_body,
        out_shape=pltpu.VMEM((rows, D), BF16),
        in_specs=[vmem] * 5,
        out_specs=vmem,
        compiler_params=pltpu.CompilerParams(vmem_limit_bytes=12 * 2**20),
        name="mlp",
    )(stream, own, other, gain, in_vmem(w))


def part(ref, start, count):
    return ref[:, pl.ds(start, count), :].reshape(NX * count, ref.shape[-1])


def near_head_body(
    stream_ref, own1_ref, other1_ref, own2_ref, other2_ref, turn_hbm, plain_hbm, near_hbm,
    rest_ref, skip_ref, pre0_ref, pre1_ref, turn_ref, plain_ref, near_ref, sems,
):
    half = D // NC
    each = half // NX
    load_turn = pltpu.make_async_copy(turn_hbm, turn_ref, sems.at[0])
    load_near = pltpu.make_async_copy(near_hbm.at[:, pl.ds(0, 2 * each), :], near_ref, sems.at[1])
    load_plain = pltpu.make_async_copy(plain_hbm, plain_ref, sems.at[2])
    load_turn.start()
    load_near.start()
    s1 = stream_ref[...].astype(F32) + (own1_ref[...].astype(F32) + other1_ref[...].astype(F32))
    s2 = (s1 + (own2_ref[...].astype(F32) + other2_ref[...].astype(F32))).astype(BF16)
    load_turn.wait()
    load_plain.start()
    turned = dot(s2, turn_ref[...]).astype(BF16)
    rest_ref[...] = turned[:, half:]
    load_near.wait()
    pre0_ref[...] = dot(turned[:, :half], part(near_ref, 0, each))
    pre1_ref[...] = dot(turned[:, :half], part(near_ref, each, each))
    load_plain.wait()
    skip_ref[...] = dot(s2, plain_ref[...]).astype(BF16)


def near_head_kernel(stream, own1, other1, own2, other2, turn, plain, near):
    rows = stream.shape[0]
    width = near.shape[-1]
    vmem = pl.BlockSpec(memory_space=pltpu.VMEM)
    return pl.pallas_call(
        near_head_body,
        out_shape=(
            pltpu.VMEM((rows, D // NC), BF16),
            pltpu.VMEM((rows, D), BF16),
            pltpu.VMEM((rows, width), F32),
            pltpu.VMEM((rows, width), F32),
        ),
        in_specs=[vmem] * 5 + [pl.BlockSpec(memory_space=pltpu.HBM)] * 3,
        out_specs=(vmem,) * 4,
        scratch_shapes=[
            pltpu.VMEM(turn.shape, BF16),
            pltpu.VMEM(plain.shape, BF16),
            pltpu.VMEM((NX, near.shape[1] // 2, width), BF16),
            pltpu.SemaphoreType.DMA((3,)),
        ],
        compiler_params=pltpu.CompilerParams(vmem_limit_bytes=24 * 2**20),
        name="near_head",
    )(stream, own1, other1, own2, other2, in_hbm(turn), in_hbm(plain), in_hbm(near))


def head_body(
    rest_ref, skip_ref, pre0_ref, pre1_ref, far_ref, last_hbm, near_hbm,
    out_ref, last_buf, near_ref, sems,
):
    width = near_ref.shape[-1]
    each = D // NC // NX
    load_near = pltpu.make_async_copy(
        near_hbm.at[:, pl.ds(2 * each, 2 * each), :], near_ref, sems.at[0]
    )
    load_last = pltpu.make_async_copy(last_hbm, last_buf, sems.at[1])
    load_near.start()
    load_last.start()

    def hidden(pre_ref, start):
        pre = pre_ref[...] + dot(rest_ref[...], part(far_ref, start, each))
        return (pre / (1.0 + jnp.exp(-pre))).astype(BF16)

    act = (hidden(pre0_ref, 0), hidden(pre1_ref, each))
    skip = (skip_ref[:, :width], skip_ref[:, width:])
    load_near.wait()
    out = []
    for ref, start in ((near_ref, 0), (far_ref, 2 * each)):
        total = None
        for k in range(2):
            at = start + k * (each // 2)
            term = dot_t(act[k], part(ref, at, each // 2))
            term = term + dot_t(skip[k], part(ref, at + each, each // 2))
            total = term if total is None else total + term
        out.append(total)
    out = jnp.concatenate(out, axis=1)
    high = out.astype(BF16)
    low = (out - high.astype(F32)).astype(BF16)
    load_last.wait()
    out_ref[...] = dot(high, last_buf[...]) + dot(low, last_buf[...])


def head_kernel(rest, skip, pre0, pre1, far, last, near):
    rows = rest.shape[0]
    width = near.shape[-1]
    vmem = pl.BlockSpec(memory_space=pltpu.VMEM)
    hbm = pl.BlockSpec(memory_space=pltpu.HBM)
    return pl.pallas_call(
        head_body,
        out_shape=jax.ShapeDtypeStruct((rows, width), F32),
        in_specs=[vmem] * 5 + [hbm] * 2,
        out_specs=vmem,
        scratch_shapes=[
            pltpu.VMEM(last.shape, BF16),
            pltpu.VMEM((NX, near.shape[1] // 2, width), BF16),
            pltpu.SemaphoreType.DMA((2,)),
        ],
        compiler_params=pltpu.CompilerParams(vmem_limit_bytes=12 * 2**20),
        name="head",
    )(rest, skip, pre0, pre1, in_vmem(far), in_hbm(last), in_hbm(near))


def rms_scale(values, gain):
    meansq = jnp.mean(values * values, axis=-1, keepdims=True)
    return values * lax.rsqrt(meansq + 1e-06) * gain


def swap(array):
    return lax.ppermute(array, "mp", [(0, 1), (1, 0)])


def per_device(
    new_embed,
    context_key_cache,
    value_cache,
    valid,
    attn_gain,
    mlp_gain,
    query_scale,
    w_qkv,
    w_out,
    w_up,
    w_down,
    head_hidden,
    final_layer_matrices,
):
    rows, _, width = context_key_cache.shape
    heads = width // HD
    piece = np.arange(PIECE)
    core, mp = lax.axis_index("c"), lax.axis_index("mp")
    second = padded_rows(
        [head_hidden, jnp.transpose(final_layer_matrices, (0, 2, 1)).reshape(2 * PIECE, width)]
    )
    first = padded_rows(
        [jnp.transpose(w_qkv, (1, 0, 2)).reshape(3 * PIECE, width), w_out.T, w_up, w_down.T]
    )
    places = np.stack([piece * 3 + b for b in range(3)] + [piece + PIECE * b for b in range(3, 6)])
    shared = from_all(first, "zh").reshape(-1, width)
    shared = from_all(shared, "x").reshape(-1, width)
    shared2 = from_all(second, ("y", "mp")).reshape(-1, width)
    pick = one_hot(matrix_rows(places, first.shape[0]), shared.shape[0])
    block1 = dot(pick, shared).astype(BF16)
    order = jnp.asarray(feature_order())
    all1 = lax.all_gather(block1, ("y", "c"), axis=0)
    _, shared2, new_embed, order = lax.optimization_barrier(
        (block1, shared2, new_embed, order)
    )
    src, step = first_rows(second.shape[0])
    pick = one_hot(jnp.asarray(src) + jnp.asarray(step) * mp, shared2.shape[0])
    shared2 = dot(pick, shared2).astype(BF16)
    shared2 = from_all(shared2, "zh").reshape(-1, width)
    block2 = dot(one_hot(second_rows(), shared2.shape[0]), shared2).astype(BF16)

    half = jnp.asarray(half_order())
    order2 = jnp.concatenate([half + PIECE * core, half + PIECE * (1 - core)])
    outs = jnp.asarray(output_order())
    outs = jnp.concatenate([outs + PIECE * core, outs + PIECE * (1 - core)])
    ids = jnp.arange(D, dtype=jnp.int32)
    forth = (ids[:, None] == order[None, :]).astype(BF16)
    turn = (order[:, None] == order2[None, :]).astype(BF16)
    plain = (order[:, None] == ids[None, :]).astype(BF16)
    last = (outs[:, None] == ids[None, : D // 2]).astype(BF16)

    normed = rms_scale(new_embed.astype(F32), attn_gain).astype(BF16)
    both = dot(jnp.concatenate([normed, new_embed], axis=0), forth).astype(BF16)
    normed_o, stream_o = both[:rows], both[rows:]
    gain_o = mlp_gain.reshape(NY, NZ, NX, NC, PIECE).transpose(0, 3, 1, 2, 4).reshape(1, D)
    pool = (jnp.arange(width)[:, None] // HD == jnp.arange(128)[None, :]).astype(BF16)
    scale = jnp.tile(query_scale, heads).reshape(1, width)
    used = jnp.broadcast_to(valid[:, None], (rows, 128))
    normed_o, stream_o, gain_o, pool, scale, used, turn, plain, last, block2 = (
        lax.optimization_barrier(
            (normed_o, stream_o, gain_o, pool, scale, used, turn, plain, last, block2)
        )
    )
    near = from_all(block2, "x")
    far = lax.ppermute(near, "c", [(0, 1), (1, 0)])

    part1, feed_w = attention_kernel(
        normed_o, scale, used, pool, context_key_cache, value_cache, all1
    )
    other1 = swap(part1)
    part2 = mlp_kernel(stream_o, part1, other1, gain_o, feed_w)
    other2 = swap(part2)
    rest, skip, pre0, pre1 = near_head_kernel(
        stream_o, part1, other1, part2, other2, turn, plain, near
    )
    return head_kernel(rest, skip, pre0, pre1, far, last, near)


def solution(mesh):
    split = Mesh(
        mesh.devices.reshape(NY, NZ, NX, NC, mesh.shape["mp"]), ("y", "zh", "x", "c", "mp")
    )

    return jax.shard_map(
        per_device,
        mesh=split,
        in_specs=(
            P(DP, None),
            P(DP, None, "mp"),
            P(DP, None, "mp"),
            P(DP),
            P(),
            P(),
            P(),
            P(None, DP, "mp"),
            P("mp", DP),
            P(DP, "mp"),
            P("mp", DP),
            P(DP, "mp"),
            P(None, "mp", DP),
        ),
        out_specs=P(DP, "mp"),
        check_vma=False,
    )
```
